256 devices in a mesh: aux: 16 (over z, core), vir: 8 (over x, y_lo), outer: 2 (over y_hi).
Axes of the slice: x: 4, y: 4 (y_hi: 2, y_lo: 2; y = y_hi * 2 + y_lo), z: 8, core: 2. Of those that a mesh axis runs over, the one named last changes fastest.
Arguments:
- factors: bfloat16 [256, 256, 2048], P(('aux', 'outer'), None, 'vir'), may hold values from -0.125 to 0.125
- trials: float32 [16, 256, 2048], P('vir', None, 'aux'), may hold values from -6 to 6
Outputs:
- sigma: float32 [16, 256, 2048], P('vir', 'outer', 'aux')
The draws below stay inside these ranges and needn't reach their ends.
All inputs are finite; a program needn't handle non-finite values.
Results may differ from the reference program's by a relative error of at most 0.004.
Values may be sent and summed in bfloat16 or wider, within the bound.
A program may use at most 64 MiB of HBM per device.

```python
import jax
import jax.numpy as jnp
from jax import lax

O = 256
V = 2048
AUXF = 256
TRIALS = 16


def shard_levels(own_key, shape, pieces, low, top_value):
    def one(dim, shards_of):
        draws = jax.random.uniform(jax.random.fold_in(jax.random.fold_in(own_key, 6), dim), (shards_of,), jnp.float32, low / len(pieces), top_value / len(pieces))
        return jnp.repeat(jnp.exp(draws), shape[dim] // shards_of).reshape((-1,) + (1,) * (len(shape) - dim - 1))

    level = one(*pieces[0])
    for cut in pieces[1:]:
        level = level * one(*cut)
    return level


def centred(key, dims, spread, bound, pieces=(), held_as=jnp.bfloat16):
    entries = jax.random.normal(key, dims, jnp.float32) * spread
    if len(pieces) > 0:
        entries = shard_levels(key, dims, pieces, -0.22, 0.18) * entries
    return jnp.clip(entries, min=-bound, max=bound).astype(held_as)


def setup_inputs(seed: int = 0) -> dict:
    key_list = jax.random.split(jax.random.key(seed), 3)
    return {
        "factors": centred(key_list[0], (AUXF, O, V), V ** -0.5, 0.125, ((0, 32), (2, 8))),
        "trials": centred(key_list[1], (TRIALS, O, V), 1.0, 6.0, ((0, 8), (2, 16)), jnp.float32),
    }


def reference(factors, trials):
    whole = factors.astype(jnp.float32)
    trial_b = trials.astype(jnp.bfloat16)

    def single(vector):
        vec32 = vector.astype(jnp.float32)
        pair = jnp.einsum("qib,jb->qij", whole, vec32).astype(jnp.bfloat16)
        pair = lax.optimization_barrier(pair).astype(jnp.float32)
        return jnp.einsum("qij,qja->ia", pair, whole)

    return lax.map(single, trial_b)
```

```python
import jax
import jax.numpy as jnp
from jax import lax
from jax.experimental import pallas as pl
from jax.experimental.pallas import tpu as pltpu
from jax.sharding import Mesh
from jax.sharding import PartitionSpec as P

MESH = pl.DeviceIdType.MESH
BF, F32 = jnp.bfloat16, jnp.float32
NX, NZ, NK = 4, 8, 4
RIGHT = ("o0", "o1", "o2", "f0", "f1", "y0", "f2", "y1", "o3", "y2", "f3", "y3")
LEFT = ("o0", "o1", "o2", "y0", "y1", "f0", "y2", "f1", "y3", "f2", "o3", "f3")
RIGHT_AT = (0, 0, 0, 1, 2, 3, 4, 5, 6, 7, 9, 9)
LEFT_AT = (0, 0, 0, 2, 3, 4, 4, 5, 6, 7, 8, 9)
Y_AT = (2, 3, 4, 5)


def kernel(f_ref, x_ref, o_ref, fb, xb, xs, sig, p32, pb, rs, rr, yb, yr, tot,
           s_loc, s_xa, r_xa, s_y, r_y, s_x, r_x, s_d, r_d, s_z, r_z, s_rs, r_rs, s_o, r_o):
    z, c, x = lax.axis_index("z"), lax.axis_index("core"), lax.axis_index("x")
    ylo, yhi = lax.axis_index("ylo"), lax.axis_index("yhi")
    oc, oy, oh = 1 - c, 1 - ylo, 1 - yhi
    xr, xl = lax.rem(x + 1, NX), lax.rem(x + NX - 1, NX)
    zr, zl = lax.rem(z + 1, NZ), lax.rem(z + NZ - 1, NZ)

    column = []
    for d in range(1, 8):
        column.append((d & 1, (d >> 1) & 1, d >> 2))

    def at(d):
        return {"core": lax.rem(c + d[0], 2), "ylo": lax.rem(ylo + d[1], 2), "yhi": lax.rem(yhi + d[2], 2)}

    partners = [{"x": xr}, {"x": xl}, {"z": zr}, {"z": zl}] + [at(d) for d in column]
    barrier = pltpu.get_barrier_semaphore()
    for partner in partners:
        pl.semaphore_signal(barrier, inc=1, device_id=partner, device_id_type=MESH)

    started = []

    def send(src, dst, ssem, rsem, device):
        copy = pltpu.make_async_remote_copy(
            src_ref=src, dst_ref=dst, send_sem=ssem, recv_sem=rsem, device_id=device, device_id_type=MESH)
        copy.start()
        started.append(copy)
        return copy

    def landed(ref, rsem, device):
        pltpu.make_async_remote_copy(
            src_ref=ref, dst_ref=ref, send_sem=rsem, recv_sem=rsem, device_id=device, device_id_type=MESH).wait_recv()

    v, vy = 2 * x + ylo, 2 * x + oy
    local = [pltpu.make_async_copy(f_ref.at[4 * ylo + k], fb.at[v, 2 * k], s_loc.at[k]) for k in range(NK)]
    for copy in local:
        copy.start()
    mine = pl.ds(pl.multiple_of(c * 128, 128), 128)
    xs[...] = x_ref[...].astype(BF)
    xb[z, ylo, :, mine] = x_ref[c].astype(BF)
    pl.semaphore_wait(barrier, len(partners))

    place = xb.at[z, ylo, :, mine]
    send(xs.at[c], place, s_xa.at[0], r_xa.at[0], {"ylo": oy})
    send(xs.at[oc], place, s_xa.at[1], r_xa.at[1], {"ylo": oy, "core": oc})
    send(xs.at[oc], place, s_xa.at[2], r_xa.at[2], {"core": oc})
    for k in range(NK):
        send(f_ref.at[4 * oy + k], fb.at[v, 2 * k], s_y.at[k], r_y.at[k], {"ylo": oy})

    def place_x(direction, kind, k, at_x):
        if kind == "o":
            return fb.at[2 * at_x + ylo, 2 * k]
        if kind == "y":
            return fb.at[2 * at_x + oy, 2 * k]
        if direction == 0:
            return fb.at[2 * lax.rem(at_x + NX - 1, NX) + ylo, 2 * k]
        return fb.at[2 * lax.rem(at_x + 1, NX) + oy, 2 * k]

    def send_x(direction, n):
        kind, k = (RIGHT, LEFT)[direction][n][0], int((RIGHT, LEFT)[direction][n][1])
        chunk = place_x(direction, kind, k, x)
        send(chunk, chunk, s_x.at[direction, n], r_x.at[direction, n], {"x": (xr, xl)[direction]})

    count = [0] * NK

    def across(s, k):
        send(fb.at[s, 2 * k], fb.at[s, 2 * k + 1], s_d.at[k, count[k]], r_d.at[k], {"core": oc})
        count[k] += 1

    def land_x(direction, n):
        kind, k = (RIGHT, LEFT)[direction][n][0], int((RIGHT, LEFT)[direction][n][1])
        sender = (xl, xr)[direction]
        landed(place_x(direction, kind, k, sender), r_x.at[direction, n], {"x": sender})
        if kind == "o":
            s = 2 * sender + ylo
        elif kind == "y":
            s = 2 * sender + oy
        else:
            s = 2 * lax.rem(x + 2, NX) + (ylo, oy)[direction]
        across(s, k)

    def send_z(direction, i):
        if direction == 0:
            chunk = xb.at[lax.rem(z + NZ - i // 2, NZ), i % 2]
        else:
            chunk = xb.at[lax.rem(z + i // 2, NZ), 1 - i % 2]
        send(chunk, chunk, s_z.at[direction, i], r_z.at[direction, i], {"z": (zr, zl)[direction]})

    def land_z(i):
        landed(xb.at[lax.rem(z + NZ - 1 - i // 2, NZ), i % 2], r_z.at[0, i], {"z": zl})
        if i < 5:
            send_z(0, i + 2)
        landed(xb.at[lax.rem(z + 1 + i // 2, NZ), 1 - i % 2], r_z.at[1, i], {"z": zr})
        if i < 5:
            send_z(1, i + 2)

    def tick(n):
        if n:
            land_x(0, n - 1)
            land_x(1, n - 1)
        for k in range(NK):
            if Y_AT[k] == n:
                landed(fb.at[vy, 2 * k], r_y.at[k], {"ylo": oy})
                across(vy, k)
        for m in range(12):
            if RIGHT_AT[m] == n:
                send_x(0, m)
            if LEFT_AT[m] == n:
                send_x(1, m)

    def mm1(k):
        landed(fb.at[:, 2 * k + 1], r_d.at[k], {"core": oc})
        p32[...] = jnp.zeros_like(p32)

        @pl.loop(0, 8)
        def _(s):
            p32[...] += lax.dot_general(
                fb[s, 2 * k:2 * k + 2].reshape(512, 256), xb[s].reshape(512, 256),
                (((1,), (1,)), ((), ())), preferred_element_type=F32)

        for q in range(2):
            for m in range(2):
                pb[256 * m:256 * m + 256, 256 * q:256 * q + 256] = (
                    p32[256 * q:256 * q + 256, 256 * m:256 * m + 256].astype(BF))

    def mm2_block(k, s):
        part = jnp.dot(pb[...], fb[s, 2 * k:2 * k + 2].reshape(512, 256), preferred_element_type=F32)
        sig[s] = part if k == 0 else sig[s] + part

    def mm2(k):
        @pl.loop(0, 8)
        def _(s):
            mm2_block(k, s)

    for k in range(NK):
        local[k].wait()
        across(v, k)
        if k == 2:
            tick(0)
    landed(xb.at[z, ylo, :, pl.ds(pl.multiple_of(oc * 128, 128), 128)], r_xa.at[2], {"core": oc})
    landed(xb.at[z, oy, :, mine], r_xa.at[0], {"ylo": oy})
    landed(xb.at[z, oy, :, pl.ds(pl.multiple_of(oc * 128, 128), 128)], r_xa.at[1], {"ylo": oy, "core": oc})
    for i in range(2):
        send_z(0, i)
        send_z(1, i)
    for n in range(1, 13):
        tick(n)
        if 3 <= n <= 9:
            land_z(n - 3)
        if 9 <= n < 12:
            mm1(n - 9)
            mm2(n - 9)

    def dest(direction, i):
        hops = (4 if i % 2 == 0 else 3) - i // 2
        slot = i % 2 if direction == 0 else 1 - i % 2
        return lax.rem(z + (hops if direction == 0 else NZ - hops), NZ), slot

    def pass_on(i):
        for direction in range(2):
            block, slot = dest(direction, i)
            own = sig[block, 256 * slot:256 * slot + 256]
            if i >= 2:
                landed(rr.at[direction, i - 2], r_rs.at[direction, i - 2], {"z": (zl, zr)[direction]})
                own = own + rr[direction, i - 2].astype(F32)
            rs[direction, i] = own.astype(BF)
            send(rs.at[direction, i], rr.at[direction, i], s_rs.at[direction, i], r_rs.at[direction, i],
                 {"z": (zr, zl)[direction]})

    mm1(3)
    mm2_block(3, lax.rem(z + 4, NZ))
    pass_on(0)
    mm2_block(3, lax.rem(z + 3, NZ))
    mm2_block(3, lax.rem(z + 5, NZ))
    pass_on(1)

    @pl.loop(0, 5)
    def _(n):
        mm2_block(3, lax.rem(z + 6 + n, NZ))

    for i in range(2, 7):
        pass_on(i)
    for direction in range(2):
        for i in (5, 6):
            landed(rr.at[direction, i], r_rs.at[direction, i], {"z": (zl, zr)[direction]})
    tot[0] = sig[z, :256] + rr[0, 6].astype(F32) + rr[1, 5].astype(F32)
    tot[1] = sig[z, 256:] + rr[0, 5].astype(F32) + rr[1, 6].astype(F32)
    for slot in range(2):
        for half in range(2):
            for cols in range(2):
                yb[slot, half, cols] = (
                    tot[slot, 128 * half:128 * half + 128, 128 * cols:128 * cols + 128].astype(BF))
    last = []
    for n, d in enumerate(column):
        there = at(d)
        send(yb.at[there["ylo"], there["yhi"], there["core"]], yr.at[c, ylo, yhi], s_o.at[n], r_o.at[n], there)
    yr[c, ylo, yhi] = yb[ylo, yhi, c]
    for n, d in enumerate(column):
        there = at(d)
        landed(yr.at[there["core"], there["ylo"], there["yhi"]], r_o.at[n], there)
    for t in range(2):
        o_ref[t] = (yr[t, 0, 0].astype(F32) + yr[t, 0, 1].astype(F32)) + (
            yr[t, 1, 0].astype(F32) + yr[t, 1, 1].astype(F32))
    for copy in started:
        copy.wait_send()


def per_device(factors, trials):
    dma = pltpu.SemaphoreType.DMA
    return pl.pallas_call(
        kernel,
        out_shape=jax.ShapeDtypeStruct((2, 128, 128), F32),
        in_specs=[pl.BlockSpec(memory_space=pl.ANY), pl.BlockSpec(memory_space=pltpu.VMEM)],
        out_specs=pl.BlockSpec(memory_space=pltpu.VMEM),
        scratch_shapes=[
            pltpu.VMEM((8, 8, 256, 256), BF),
            pltpu.VMEM((8, 2, 256, 256), BF),
            pltpu.VMEM((2, 256, 128), BF),
            pltpu.VMEM((8, 512, 256), F32),
            pltpu.VMEM((512, 512), F32),
            pltpu.VMEM((512, 512), BF),
            pltpu.VMEM((2, 7, 256, 256), BF),
            pltpu.VMEM((2, 7, 256, 256), BF),
            pltpu.VMEM((2, 2, 2, 128, 128), BF),
            pltpu.VMEM((2, 2, 2, 128, 128), BF),
            pltpu.VMEM((2, 256, 256), F32),
            dma((4,)), dma((3,)), dma((3,)), dma((4,)), dma((4,)), dma((2, 12)), dma((2, 12)),
            dma((4, 8)), dma((4,)), dma((2, 7)), dma((2, 7)), dma((2, 7)), dma((2, 7)), dma((7,)), dma((7,)),
        ],
        compiler_params=pltpu.CompilerParams(
            collective_id=0, has_side_effects=True, vmem_limit_bytes=60000 * 1024),
    )(factors, trials)


def solution(mesh):
    torus = Mesh(mesh.devices.reshape(NZ, 2, NX, 2, 2), ("z", "core", "x", "ylo", "yhi"))
    in_specs = (P(("z", "core", "yhi"), None, ("x", "ylo")), P(("x", "ylo"), None, ("z", "core")))
    out_specs = P(("x", "ylo"), "yhi", ("z", "core"))
    return jax.shard_map(
        per_device, mesh=torus, in_specs=in_specs, out_specs=out_specs, check_vma=False
    )
```

```python
import jax
import jax.numpy as jnp
from jax import lax
from jax.experimental import pallas as pl
from jax.experimental.pallas import tpu as pltpu
from jax.sharding import Mesh
from jax.sharding import PartitionSpec as P

MESH = pl.DeviceIdType.MESH
BF, F32 = jnp.bfloat16, jnp.float32
NX, NZ, NK = 4, 8, 4
RIGHT = ("o0", "o1", "o2", "f0", "f1", "y0", "f2", "y1", "o3", "y2", "f3", "y3")
LEFT = ("o0", "o1", "o2", "y0", "y1", "f0", "y2", "f1", "y3", "f2", "o3", "f3")
RIGHT_AT = (0, 0, 0, 1, 2, 3, 4, 5, 6, 7, 9, 9)
LEFT_AT = (0, 0, 0, 2, 3, 4, 4, 5, 6, 7, 8, 9)
Y_AT = (2, 3, 4, 5)
BLOCKS = (4, 3, 5, 2, 6, 1, 7, 0)
GROUPS = ((0, 1), (1, 3), (3, 5), (5, 8))


def kernel(f_ref, x_ref, o_ref, fb, xb, xs, sig, p32, pb, as_, ar, y1s, y1r, y2s, y2r, yb, bs, br, tot, ys, yr, give, take,
           s_loc, s_xa, r_xa, s_y, r_y, s_x, r_x, s_d, r_d, s_z, r_z, s_a, r_a, s_y1, r_y1, s_y2, r_y2, s_b, r_b, s_o, r_o):
    z, c, x = lax.axis_index("z"), lax.axis_index("core"), lax.axis_index("x")
    ylo, yhi = lax.axis_index("ylo"), lax.axis_index("yhi")
    oc, oy, oh = 1 - c, 1 - ylo, 1 - yhi
    xr, xl = lax.rem(x + 1, NX), lax.rem(x + NX - 1, NX)
    zr, zl = lax.rem(z + 1, NZ), lax.rem(z + NZ - 1, NZ)

    partners = [{"x": xr}, {"x": xl}, {"z": zr}, {"z": zl}, {"core": oc}, {"ylo": oy}, {"ylo": oy, "core": oc},
                {"ylo": oy, "yhi": oh}, {"yhi": oh}]
    barrier = pltpu.get_barrier_semaphore()
    for partner in partners:
        pl.semaphore_signal(barrier, inc=1, device_id=partner, device_id_type=MESH)

    started = []

    def send(src, dst, ssem, rsem, device):
        copy = pltpu.make_async_remote_copy(
            src_ref=src, dst_ref=dst, send_sem=ssem, recv_sem=rsem, device_id=device, device_id_type=MESH)
        copy.start()
        started.append(copy)
        return copy

    def landed(ref, rsem, device):
        pltpu.make_async_remote_copy(
            src_ref=ref, dst_ref=ref, send_sem=rsem, recv_sem=rsem, device_id=device, device_id_type=MESH).wait_recv()

    v, vy = 2 * x + ylo, 2 * x + oy
    local = [pltpu.make_async_copy(f_ref.at[4 * ylo + k], fb.at[v, 2 * k], s_loc.at[k]) for k in range(NK)]
    for copy in local:
        copy.start()
    mine = pl.ds(pl.multiple_of(c * 128, 128), 128)
    xs[...] = x_ref[...].astype(BF)
    xb[z, ylo, :, mine] = x_ref[c].astype(BF)
    pl.semaphore_wait(barrier, len(partners))

    place = xb.at[z, ylo, :, mine]
    send(xs.at[c], place, s_xa.at[0], r_xa.at[0], {"ylo": oy})
    send(xs.at[oc], place, s_xa.at[1], r_xa.at[1], {"ylo": oy, "core": oc})
    send(xs.at[oc], place, s_xa.at[2], r_xa.at[2], {"core": oc})
    for k in range(NK):
        send(f_ref.at[4 * oy + k], fb.at[v, 2 * k], s_y.at[k], r_y.at[k], {"ylo": oy})

    def place_x(direction, kind, k, at_x):
        if kind == "o":
            return fb.at[2 * at_x + ylo, 2 * k]
        if kind == "y":
            return fb.at[2 * at_x + oy, 2 * k]
        if direction == 0:
            return fb.at[2 * lax.rem(at_x + NX - 1, NX) + ylo, 2 * k]
        return fb.at[2 * lax.rem(at_x + 1, NX) + oy, 2 * k]

    def send_x(direction, n):
        kind, k = (RIGHT, LEFT)[direction][n][0], int((RIGHT, LEFT)[direction][n][1])
        chunk = place_x(direction, kind, k, x)
        send(chunk, chunk, s_x.at[direction, n], r_x.at[direction, n], {"x": (xr, xl)[direction]})

    count = [0] * NK

    def across(s, k):
        send(fb.at[s, 2 * k], fb.at[s, 2 * k + 1], s_d.at[k, count[k]], r_d.at[k], {"core": oc})
        count[k] += 1

    def land_x(direction, n):
        kind, k = (RIGHT, LEFT)[direction][n][0], int((RIGHT, LEFT)[direction][n][1])
        sender = (xl, xr)[direction]
        landed(place_x(direction, kind, k, sender), r_x.at[direction, n], {"x": sender})
        if kind == "o":
            s = 2 * sender + ylo
        elif kind == "y":
            s = 2 * sender + oy
        else:
            s = 2 * lax.rem(x + 2, NX) + (ylo, oy)[direction]
        across(s, k)

    def send_z(direction, i):
        if direction == 0:
            chunk = xb.at[lax.rem(z + NZ - i // 2, NZ), i % 2]
        else:
            chunk = xb.at[lax.rem(z + i // 2, NZ), 1 - i % 2]
        send(chunk, chunk, s_z.at[direction, i], r_z.at[direction, i], {"z": (zr, zl)[direction]})

    def land_z(i):
        landed(xb.at[lax.rem(z + NZ - 1 - i // 2, NZ), i % 2], r_z.at[0, i], {"z": zl})
        if i < 5:
            send_z(0, i + 2)
        landed(xb.at[lax.rem(z + 1 + i // 2, NZ), 1 - i % 2], r_z.at[1, i], {"z": zr})
        if i < 5:
            send_z(1, i + 2)

    def tick(n):
        if n:
            land_x(0, n - 1)
            land_x(1, n - 1)
        for k in range(NK):
            if Y_AT[k] == n:
                landed(fb.at[vy, 2 * k], r_y.at[k], {"ylo": oy})
                across(vy, k)
        for m in range(12):
            if RIGHT_AT[m] == n:
                send_x(0, m)
            if LEFT_AT[m] == n:
                send_x(1, m)

    def mm1(k):
        landed(fb.at[:, 2 * k + 1], r_d.at[k], {"core": oc})
        total = None
        for s in range(8):
            part = lax.dot_general(
                fb[s, 2 * k:2 * k + 2].reshape(512, 256), xb[s].reshape(512, 256),
                (((1,), (1,)), ((), ())), preferred_element_type=F32)
            total = part if s == 0 else total + part
        p32[...] = total
        for q in range(2):
            for m in range(2):
                pb[256 * m:256 * m + 256, 256 * q:256 * q + 256] = (
                    p32[256 * q:256 * q + 256, 256 * m:256 * m + 256].astype(BF))

    def mm2_block(k, s):
        part = jnp.dot(pb[...], fb[s, 2 * k:2 * k + 2].reshape(512, 256), preferred_element_type=F32)
        part = part.reshape(2, 2, 128, 256)
        sig[s] = part if k == 0 else sig[s] + part

    def mm2(k):
        for s in range(8):
            mm2_block(k, s)

    for k in range(NK):
        local[k].wait()
        across(v, k)
        if k == 2:
            tick(0)
    landed(xb.at[z, ylo, :, pl.ds(pl.multiple_of(oc * 128, 128), 128)], r_xa.at[2], {"core": oc})
    landed(xb.at[z, oy, :, mine], r_xa.at[0], {"ylo": oy})
    landed(xb.at[z, oy, :, pl.ds(pl.multiple_of(oc * 128, 128), 128)], r_xa.at[1], {"ylo": oy, "core": oc})
    for i in range(2):
        send_z(0, i)
        send_z(1, i)
    for n in range(1, 13):
        tick(n)
        if 3 <= n <= 9:
            land_z(n - 3)
        if 9 <= n < 12:
            mm1(n - 9)
            mm2(n - 9)

    right = {"ylo": oy, "yhi": lax.rem(yhi + ylo, 2)}
    left = {"ylo": oy, "yhi": lax.rem(yhi + oy, 2)}
    far = {"ylo": ylo, "yhi": oh}
    sides = (right, left)
    rings = ({"z": zr}, {"z": zl})
    theirs = pl.ds(pl.multiple_of(oc * 128, 128), 128)

    def block(n):
        return lax.rem(z + BLOCKS[n], NZ)

    def dest(direction, i):
        hops = (4 if i % 2 == 0 else 3) - i // 2
        return BLOCKS.index(hops if direction == 0 else NZ - hops), (i % 2 if direction == 0 else 1 - i % 2)

    def a_step(i):
        for d in range(2):
            n, slot = dest(d, i)
            own = sig[block(n), slot, :, :, mine].reshape(256, 128)
            if i >= 2:
                landed(ar.at[d, i - 2], r_a.at[d, i - 2], rings[1 - d])
                own = own + ar[d, i - 2].astype(F32)
            as_[d, i] = own.astype(BF)
            send(as_.at[d, i], ar.at[d, i], s_a.at[d, i], r_a.at[d, i], rings[d])

    def far_rows(n, half):
        return sig[block(n), ylo, oh, 64 * half:64 * half + 64, theirs]

    def y1(g):
        lo, hi = GROUPS[g]
        for d in range(2):
            for n in range(lo, hi):
                y1s[d, n] = far_rows(n, d).astype(BF)
            send(y1s.at[d, lo:hi], y1r.at[d, lo:hi], s_y1.at[d, g], r_y1.at[d, g], sides[d])

    def y2(g):
        lo, hi = GROUPS[g]
        for d in range(2):
            landed(y1r.at[d, lo:hi], r_y1.at[d, g], sides[1 - d])
            for n in range(lo, hi):
                for half in range(2):
                    own = sig[block(n), sides[d]["ylo"], sides[d]["yhi"], 64 * half:64 * half + 64, theirs]
                    if half == d:
                        own = own + y1r[d, n].astype(F32)
                    y2s[d, n, 64 * half:64 * half + 64] = own.astype(BF)
            send(y2s.at[d, lo:hi], y2r.at[d, lo:hi], s_y2.at[d, g], r_y2.at[d, g], sides[d])

    def y3(g):
        lo, hi = GROUPS[g]
        for d in range(2):
            landed(y2r.at[d, lo:hi], r_y2.at[d, g], sides[1 - d])
        for n in range(lo, hi):
            yb[n] = sig[block(n), ylo, yhi, :, theirs] + y2r[0, n].astype(F32) + y2r[1, n].astype(F32)

    def b_step(i):
        for d in range(2):
            n, sub = dest(d, i)
            own = yb[n, 64 * sub:64 * sub + 64]
            if i >= 2:
                landed(br.at[d, i - 2], r_b.at[d, i - 2], rings[1 - d])
                own = own + br[d, i - 2].astype(F32)
            bs[d, i] = own.astype(BF)
            send(bs.at[d, i], br.at[d, i], s_b.at[d, i], r_b.at[d, i], rings[d])

    mm1(3)
    mm2_block(3, block(0))
    a_step(0)
    y1(0)
    mm2_block(3, block(1))
    mm2_block(3, block(2))
    a_step(1)
    y1(1)
    mm2_block(3, block(3))
    mm2_block(3, block(4))
    y1(2)
    for n in (5, 6, 7):
        mm2_block(3, block(n))
    y1(3)
    y2(0)
    a_step(2)
    y2(1)
    a_step(3)
    y3(0)
    b_step(0)
    y2(2)
    a_step(4)
    y3(1)
    b_step(1)
    y2(3)
    b_step(2)
    a_step(5)
    y3(2)
    b_step(3)
    a_step(6)
    b_step(4)
    y3(3)
    b_step(5)
    b_step(6)
    for d in range(2):
        for i in (5, 6):
            landed(ar.at[d, i], r_a.at[d, i], rings[1 - d])
    for slot in range(2):
        got = ar[0, 6 - slot].astype(F32) + ar[1, 5 + slot].astype(F32)
        whole = sig[z, slot, :, :, mine] + got.reshape(2, 128, 128)
        tot[slot] = whole
        ys[slot] = whole.astype(BF)
    for n, there in enumerate((right, left, far)):
        send(ys.at[there["ylo"], there["yhi"]], yr.at[n], s_o.at[n], r_o.at[n], there)
    for d in range(2):
        for i in (5, 6):
            landed(br.at[d, i], r_b.at[d, i], rings[1 - d])
    for sub in range(2):
        give[64 * sub:64 * sub + 64] = (
            yb[7, 64 * sub:64 * sub + 64] + br[0, 6 - sub].astype(F32) + br[1, 5 + sub].astype(F32))
    send(give, take, s_o.at[3], r_o.at[3], {"core": oc})
    for n, there in enumerate((left, right, far)):
        landed(yr.at[n], r_o.at[n], there)
    o_ref[c] = (tot[ylo, yhi] + yr[0].astype(F32)) + (yr[1].astype(F32) + yr[2].astype(F32))
    landed(take, r_o.at[3], {"core": oc})
    o_ref[oc] = take[...]
    for copy in started:
        copy.wait_send()


def per_device(factors, trials):
    dma = pltpu.SemaphoreType.DMA
    return pl.pallas_call(
        kernel,
        out_shape=jax.ShapeDtypeStruct((2, 128, 128), F32),
        in_specs=[pl.BlockSpec(memory_space=pl.ANY), pl.BlockSpec(memory_space=pltpu.VMEM)],
        out_specs=pl.BlockSpec(memory_space=pltpu.VMEM),
        scratch_shapes=[
            pltpu.VMEM((8, 8, 256, 256), BF),
            pltpu.VMEM((8, 2, 256, 256), BF),
            pltpu.VMEM((2, 256, 128), BF),
            pltpu.VMEM((8, 2, 2, 128, 256), F32),
            pltpu.VMEM((512, 512), F32),
            pltpu.VMEM((512, 512), BF),
            pltpu.VMEM((2, 7, 256, 128), BF),
            pltpu.VMEM((2, 7, 256, 128), BF),
            pltpu.VMEM((2, 8, 64, 128), BF),
            pltpu.VMEM((2, 8, 64, 128), BF),
            pltpu.VMEM((2, 8, 128, 128), BF),
            pltpu.VMEM((2, 8, 128, 128), BF),
            pltpu.VMEM((8, 128, 128), F32),
            pltpu.VMEM((2, 7, 64, 128), BF),
            pltpu.VMEM((2, 7, 64, 128), BF),
            pltpu.VMEM((2, 2, 128, 128), F32),
            pltpu.VMEM((2, 2, 128, 128), BF),
            pltpu.VMEM((3, 128, 128), BF),
            pltpu.VMEM((128, 128), F32),
            pltpu.VMEM((128, 128), F32),
            dma((4,)), dma((3,)), dma((3,)), dma((4,)), dma((4,)), dma((2, 12)), dma((2, 12)),
            dma((4, 8)), dma((4,)), dma((2, 7)), dma((2, 7)), dma((2, 7)), dma((2, 7)),
            dma((2, 4)), dma((2, 4)), dma((2, 4)), dma((2, 4)), dma((2, 7)), dma((2, 7)), dma((4,)), dma((4,)),
        ],
        compiler_params=pltpu.CompilerParams(
            collective_id=0, has_side_effects=True, vmem_limit_bytes=60000 * 1024),
    )(factors, trials)


def solution(mesh):
    torus = Mesh(mesh.devices.reshape(NZ, 2, NX, 2, 2), ("z", "core", "x", "ylo", "yhi"))
    in_specs = (P(("z", "core", "yhi"), None, ("x", "ylo")), P(("x", "ylo"), None, ("z", "core")))
    out_specs = P(("x", "ylo"), "yhi", ("z", "core"))
    return jax.shard_map(
        per_device, mesh=torus, in_specs=in_specs, out_specs=out_specs, check_vma=False
    )
```

```python
import jax
import jax.numpy as jnp
from jax import lax
from jax.experimental import pallas as pl
from jax.experimental.pallas import tpu as pltpu
from jax.sharding import Mesh
from jax.sharding import PartitionSpec as P

MESH = pl.DeviceIdType.MESH
BF, F32 = jnp.bfloat16, jnp.float32
NX, NZ, NK = 4, 8, 4
RIGHT = ("o0", "o1", "o2", "f0", "f1", "y0", "f2", "y1", "o3", "y2", "f3", "y3")
LEFT = ("o0", "o1", "o2", "y0", "y1", "f0", "y2", "f1", "y3", "f2", "o3", "f3")
RIGHT_AT = (-1, -1, -1, 1, 2, 3, 4, 5, 6, 7, 9, 9)
LEFT_AT = (-1, -1, -1, 2, 3, 4, 4, 5, 6, 7, 8, 9)
Y_AT = (2, 3, 4, 5)
BLOCKS = (4, 3, 5, 2, 6, 1, 7, 0)
GROUPS = ((0, 1), (1, 3), (3, 5), (5, 8))


def kernel(f_ref, x_ref, o_ref, fb, xb, xf, xs, sig, p32, pb, as_, ar, y1s, y1r, y2s, y2r, yb, es, er, bs, br, tot, ys, yr, give, take,
           s_loc, s_xa, r_xa, r_y, s_x, r_x, s_d, r_d, s_z, r_z, s_a, r_a, s_y1, r_y1, s_y2, r_y2, s_e, s_b, r_b, s_o, s_g, r_o):
    z, c, x = lax.axis_index("z"), lax.axis_index("core"), lax.axis_index("x")
    ylo, yhi = lax.axis_index("ylo"), lax.axis_index("yhi")
    oc, oy, oh = 1 - c, 1 - ylo, 1 - yhi
    xr, xl = lax.rem(x + 1, NX), lax.rem(x + NX - 1, NX)
    zr, zl = lax.rem(z + 1, NZ), lax.rem(z + NZ - 1, NZ)

    partners = [{"z": lax.rem(z + 2, NZ)}, {"z": lax.rem(z + NZ - 2, NZ)}, {"x": xr}, {"x": xl}, {"z": zr}, {"z": zl}, {"core": oc}, {"ylo": oy}, {"ylo": oy, "core": oc},
                {"ylo": oy, "yhi": oh}, {"yhi": oh}]
    barrier = pltpu.get_barrier_semaphore()
    for partner in partners:
        pl.semaphore_signal(barrier, inc=1, device_id=partner, device_id_type=MESH)

    def send(src, dst, ssem, rsem, device):
        copy = pltpu.make_async_remote_copy(
            src_ref=src, dst_ref=dst, send_sem=ssem, recv_sem=rsem, device_id=device, device_id_type=MESH)
        copy.start()

    def landed(ref, rsem, device):
        pltpu.make_async_remote_copy(
            src_ref=ref, dst_ref=ref, send_sem=rsem, recv_sem=rsem, device_id=device, device_id_type=MESH).wait_recv()

    v, vy = 2 * x + ylo, 2 * x + oy
    local = [pltpu.make_async_copy(f_ref.at[4 * ylo + k], fb.at[v, 2 * k], s_loc.at[k]) for k in range(NK)]
    for copy in local:
        copy.start()
    mine = pl.ds(pl.multiple_of(c * 128, 128), 128)
    own_x = pltpu.make_async_copy(x_ref, xf, s_loc.at[NK])
    own_x.start()
    pl.semaphore_wait(barrier, len(partners))

    def place_x(direction, kind, k, at_x):
        if kind == "o":
            return fb.at[2 * at_x + ylo, 2 * k]
        if kind == "y":
            return fb.at[2 * at_x + oy, 2 * k]
        if direction == 0:
            return fb.at[2 * lax.rem(at_x + NX - 1, NX) + ylo, 2 * k]
        return fb.at[2 * lax.rem(at_x + 1, NX) + oy, 2 * k]

    def send_x(direction, n):
        kind, k = (RIGHT, LEFT)[direction][n][0], int((RIGHT, LEFT)[direction][n][1])
        chunk = place_x(direction, kind, k, x)
        send(chunk, chunk, s_x, r_x.at[n], {"x": (xr, xl)[direction]})

    groups = {11: 4, 12: 5}
    parts = {3: [], 4: [], 5: []}

    def across(s, k, n=0):
        group = groups.get(n, k)
        send(fb.at[s, 2 * k], fb.at[s, 2 * k + 1], s_d, r_d.at[group], {"core": oc})
        if k == NK - 1:
            parts[group].append(s)

    def land_x(direction, n):
        kind, k = (RIGHT, LEFT)[direction][n][0], int((RIGHT, LEFT)[direction][n][1])
        sender = (xl, xr)[direction]
        if kind == "o":
            s = 2 * sender + ylo
        elif kind == "y":
            s = 2 * sender + oy
        else:
            s = 2 * lax.rem(x + 2, NX) + (ylo, oy)[direction]
        across(s, k, n + 1)

    def send_z(direction, i):
        if direction == 0:
            chunk = xb.at[lax.rem(z + NZ - i // 2, NZ), i % 2]
        else:
            chunk = xb.at[lax.rem(z + i // 2, NZ), 1 - i % 2]
        send(chunk, chunk, s_z, r_z.at[i], {"z": (zr, zl)[direction]})

    def land_z(i):
        landed(xb.at[0], r_z.at[i], {"z": zl})
        if i < 5:
            send_z(0, i + 2)
            send_z(1, i + 2)

    def tick(n):
        landed(fb.at[0, 0:2], r_x.at[n - 1], {"x": xl})
        land_x(0, n - 1)
        land_x(1, n - 1)
        for k in range(NK):
            if Y_AT[k] == n:
                landed(fb.at[vy, 2 * k], r_y.at[k], {"ylo": oy})
                across(vy, k)
        for m in range(12):
            if RIGHT_AT[m] == n:
                send_x(0, m)
            if LEFT_AT[m] == n:
                send_x(1, m)

    def others_landed(k, group, slices):
        landed(fb.at[0:slices, 2 * k + 1], r_d.at[group], {"core": oc})

    def products(k, slices):
        total = None
        for s in slices:
            part = lax.dot_general(
                fb[s, 2 * k:2 * k + 2].reshape(512, 256), xb[s].reshape(512, 256),
                (((1,), (1,)), ((), ())), preferred_element_type=F32)
            total = part if total is None else total + part
        return total

    def pairs_from(total):
        for q in range(2):
            for m in range(2):
                pb[256 * m:256 * m + 256, 256 * q:256 * q + 256] = (
                    total[256 * q:256 * q + 256, 256 * m:256 * m + 256].astype(BF))

    def near(*steps):
        return [lax.rem(z + n, NZ) for n in steps]

    def mm2_block(k, s):
        part = jnp.dot(pb[...], fb[s, 2 * k:2 * k + 2].reshape(512, 256), preferred_element_type=F32)
        part = part.reshape(2, 2, 128, 256)
        sig[s] = part if k == 0 else sig[s] + part

    def mm2(k):
        for s in range(8):
            mm2_block(k, s)

    for k in range(3):
        local[k].wait()
        send_x(0, k)
        send_x(1, k)
    own_x.wait()
    xs[...] = xf[...].astype(BF)
    xb[z, ylo, :, mine] = xf[c].astype(BF)
    place = xb.at[z, ylo, :, mine]
    send(xs.at[c], place, s_xa, r_xa.at[0], {"ylo": oy})
    send(xs.at[oc], place, s_xa, r_xa.at[1], {"ylo": oy, "core": oc})
    send(xs.at[oc], place, s_xa, r_xa.at[2], {"core": oc})
    for k in range(NK):
        send(f_ref.at[4 * oy + k], fb.at[v, 2 * k], s_x, r_y.at[k], {"ylo": oy})
    local[3].wait()
    for k in range(NK):
        across(v, k)
    landed(xb.at[z, ylo, :, pl.ds(pl.multiple_of(oc * 128, 128), 128)], r_xa.at[2], {"core": oc})
    landed(xb.at[z, oy, :, mine], r_xa.at[0], {"ylo": oy})
    landed(xb.at[z, oy, :, pl.ds(pl.multiple_of(oc * 128, 128), 128)], r_xa.at[1], {"ylo": oy, "core": oc})
    for i in range(2):
        send_z(0, i)
        send_z(1, i)
    for n in range(1, 13):
        tick(n)
        if 3 <= n <= 9:
            land_z(n - 3)
        if n == 7:
            others_landed(0, 0, 8)
            p32[0] = products(0, near(0, 1, 7, 2, 6))
        if n == 8:
            others_landed(1, 1, 8)
            p32[1] = products(1, near(0, 1, 7, 2, 6, 3, 5))
        if n == 9:
            pairs_from(p32[0] + products(0, near(3, 5, 4)))
            mm2(0)
            pairs_from(p32[1] + products(1, near(4)))
        if n == 10:
            mm2(1)
            others_landed(2, 2, 8)
            pairs_from(products(2, range(8)))
        if n == 11:
            mm2(2)
            others_landed(3, 3, 4)
            p32[0] = products(3, parts[3])
            others_landed(3, 4, 2)
            p32[0] += products(3, parts[4])
    others_landed(3, 5, 2)
    pairs_from(p32[0] + products(3, parts[5]))

    right = {"ylo": oy, "yhi": lax.rem(yhi + ylo, 2)}
    left = {"ylo": oy, "yhi": lax.rem(yhi + oy, 2)}
    far = {"ylo": ylo, "yhi": oh}
    sides = (right, left)
    rings = ({"z": zr}, {"z": zl})
    theirs = pl.ds(pl.multiple_of(oc * 128, 128), 128)

    def block(n):
        return lax.rem(z + BLOCKS[n], NZ)

    def dest(direction, i):
        hops = (4 if i % 2 == 0 else 3) - i // 2
        return BLOCKS.index(hops if direction == 0 else NZ - hops), (i % 2 if direction == 0 else 1 - i % 2)

    def a_step(i):
        for half, d in ((0, 0), (0, 1), (1, 0), (1, 1)):
            n, slot = dest(d, i)
            own = sig[block(n), slot, half, :, mine]
            if i >= 2:
                if d == 0:
                    landed(ar.at[:, i - 2, half], r_a.at[i - 2, half], rings[1])
                own = own + ar[d, i - 2, half].astype(F32)
            as_[d, i, half] = own.astype(BF)
            send(as_.at[d, i, half], ar.at[d, i, half], s_a, r_a.at[i, half], rings[d])

    def far_rows(n, half):
        return sig[block(n), ylo, oh, 64 * half:64 * half + 64, theirs]

    def y1(g):
        lo, hi = GROUPS[g]
        for d in range(2):
            for n in range(lo, hi):
                y1s[d, n] = far_rows(n, d).astype(BF)
            send(y1s.at[d, lo:hi], y1r.at[d, lo:hi], s_y1, r_y1.at[g], sides[d])

    def y2(g):
        lo, hi = GROUPS[g]
        landed(y1r.at[:, lo:hi], r_y1.at[g], sides[1])
        for d in range(2):
            for n in range(lo, hi):
                for half in range(2):
                    own = sig[block(n), sides[d]["ylo"], sides[d]["yhi"], 64 * half:64 * half + 64, theirs]
                    if half == d:
                        own = own + y1r[d, n].astype(F32)
                    y2s[d, n, 64 * half:64 * half + 64] = own.astype(BF)
            send(y2s.at[d, lo:hi], y2r.at[d, lo:hi], s_y2, r_y2.at[g], sides[d])

    def y3(g):
        lo, hi = GROUPS[g]
        landed(y2r.at[:, lo:hi], r_y2.at[g], sides[1])
        for n in range(lo, hi):
            yb[n] = sig[block(n), ylo, yhi, :, theirs] + y2r[0, n].astype(F32) + y2r[1, n].astype(F32)

    two = ({"z": lax.rem(z + 2, NZ)}, {"z": lax.rem(z + NZ - 2, NZ)})

    def b_far():
        for d in range(2):
            es[d] = yb[0, 64 * d:64 * d + 64].astype(BF)
            send(es.at[d], er.at[d], s_e, r_b.at[0], two[d])

    def b_third():
        for d in range(2):
            bs[0, d] = yb[1 + d].astype(BF)
            send(bs.at[0, d], br.at[0, d], s_b, r_b.at[1], rings[d])

    def b_near():
        for d in range(2):
            bs[1, d] = yb[5 + d].astype(BF)
            send(bs.at[1, d], br.at[1, d], s_b, r_b.at[2], rings[d])

    def b_second():
        landed(er, r_b.at[0], two[0])
        landed(br.at[0], r_b.at[1], rings[0])
        for d in range(2):
            for sub in range(2):
                own = yb[3 + d, 64 * sub:64 * sub + 64] + br[0, d, 64 * sub:64 * sub + 64].astype(F32)
                if sub == d:
                    own = own + er[d].astype(F32)
                bs[2, d, 64 * sub:64 * sub + 64] = own.astype(BF)
            send(bs.at[2, d], br.at[2, d], s_b, r_b.at[3], two[d])

    mm2_block(3, block(0))
    a_step(0)
    y1(0)
    mm2_block(3, block(1))
    mm2_block(3, block(2))
    a_step(1)
    y1(1)
    mm2_block(3, block(3))
    mm2_block(3, block(4))
    y1(2)
    for n in (5, 6, 7):
        mm2_block(3, block(n))
    y1(3)
    y2(0)
    a_step(2)
    y2(1)
    a_step(3)
    y2(2)
    y2(3)
    y3(0)
    b_far()
    y3(1)
    b_third()
    a_step(4)
    y3(2)
    a_step(5)
    y3(3)
    b_near()
    a_step(6)
    b_second()
    for i in (5, 6):
        for half in range(2):
            landed(ar.at[:, i, half], r_a.at[i, half], rings[0])
    for slot in range(2):
        got = ar[0, 6 - slot].astype(F32) + ar[1, 5 + slot].astype(F32)
        whole = sig[z, slot, :, :, mine] + got
        tot[slot] = whole
        ys[slot] = whole.astype(BF)
    for n, there in enumerate((right, left, far)):
        send(ys.at[there["ylo"], there["yhi"]], yr.at[n], s_o, r_o.at[n], there)
    landed(br.at[1], r_b.at[2], rings[0])
    landed(br.at[2], r_b.at[3], two[0])
    give[...] = (yb[7] + (br[1, 0].astype(F32) + br[1, 1].astype(F32))) + (br[2, 0].astype(F32) + br[2, 1].astype(F32))
    send(give, take, s_g, r_o.at[3], {"core": oc})
    for n, there in enumerate((left, right, far)):
        landed(yr.at[n], r_o.at[n], there)
    o_ref[c] = (tot[ylo, yhi] + yr[0].astype(F32)) + (yr[1].astype(F32) + yr[2].astype(F32))
    landed(take, r_o.at[3], {"core": oc})
    o_ref[oc] = take[...]
    for ref, sem in ((xb.at[0:3, 0, :, 0:128], s_xa), (fb.at[0:7, 0:4], s_x), (fb.at[0:4], s_d), (xb.at[0:7], s_z), (as_, s_a),
                     (y1s, s_y1), (y2s, s_y2), (es, s_e), (bs, s_b), (yr, s_o), (give, s_g)):
        pltpu.make_async_remote_copy(
            src_ref=ref, dst_ref=ref, send_sem=sem, recv_sem=sem, device_id={"core": oc}, device_id_type=MESH).wait_send()


def per_device(factors, trials):
    dma = pltpu.SemaphoreType.DMA
    return pl.pallas_call(
        kernel,
        out_shape=jax.ShapeDtypeStruct((2, 128, 128), F32),
        in_specs=[pl.BlockSpec(memory_space=pl.ANY), pl.BlockSpec(memory_space=pl.ANY)],
        out_specs=pl.BlockSpec(memory_space=pltpu.VMEM),
        scratch_shapes=[
            pltpu.VMEM((8, 8, 256, 256), BF),
            pltpu.VMEM((8, 2, 256, 256), BF),
            pltpu.VMEM((2, 256, 128), F32),
            pltpu.VMEM((2, 256, 128), BF),
            pltpu.VMEM((8, 2, 2, 128, 256), F32),
            pltpu.VMEM((2, 512, 512), F32),
            pltpu.VMEM((512, 512), BF),
            pltpu.VMEM((2, 7, 2, 128, 128), BF),
            pltpu.VMEM((2, 7, 2, 128, 128), BF),
            pltpu.VMEM((2, 8, 64, 128), BF),
            pltpu.VMEM((2, 8, 64, 128), BF),
            pltpu.VMEM((2, 8, 128, 128), BF),
            pltpu.VMEM((2, 8, 128, 128), BF),
            pltpu.VMEM((8, 128, 128), F32),
            pltpu.VMEM((2, 64, 128), BF),
            pltpu.VMEM((2, 64, 128), BF),
            pltpu.VMEM((3, 2, 128, 128), BF),
            pltpu.VMEM((3, 2, 128, 128), BF),
            pltpu.VMEM((2, 2, 128, 128), F32),
            pltpu.VMEM((2, 2, 128, 128), BF),
            pltpu.VMEM((3, 128, 128), BF),
            pltpu.VMEM((128, 128), F32),
            pltpu.VMEM((128, 128), F32),
            dma((5,)), dma(()), dma((3,)), dma((4,)), dma(()), dma((12,)),
            dma(()), dma((6,)), dma(()), dma((7,)), dma(()), dma((7, 2)),
            dma(()), dma((4,)), dma(()), dma((4,)), dma(()), dma(()), dma((4,)), dma(()), dma(()), dma((4,)),
        ],
        compiler_params=pltpu.CompilerParams(
            collective_id=0, has_side_effects=True, vmem_limit_bytes=60000 * 1024),
    )(factors, trials)


def solution(mesh):
    torus = Mesh(mesh.devices.reshape(NZ, 2, NX, 2, 2), ("z", "core", "x", "ylo", "yhi"))
    in_specs = (P(("z", "core", "yhi"), None, ("x", "ylo")), P(("x", "ylo"), None, ("z", "core")))
    out_specs = P(("x", "ylo"), "yhi", ("z", "core"))
    return jax.shard_map(
        per_device, mesh=torus, in_specs=in_specs, out_specs=out_specs, check_vma=False
    )
```

```python
import jax
import jax.numpy as jnp
from jax import lax
from jax.experimental import pallas as pl
from jax.experimental.pallas import tpu as pltpu
from jax.sharding import Mesh
from jax.sharding import PartitionSpec as P

MESH = pl.DeviceIdType.MESH
BF, F32 = jnp.bfloat16, jnp.float32
NX, NZ, NK = 4, 8, 4
RIGHT = ("o0", "o1", "o2", "f0", "f1", "y0", "f2", "y1", "o3", "y2", "f3", "y3")
LEFT = ("o0", "o1", "o2", "y0", "y1", "f0", "y2", "f1", "y3", "f2", "o3", "f3")
RIGHT_AT = (-1, -1, -1, 1, 2, 3, 4, 5, 6, 7, 9, 9)
LEFT_AT = (-1, -1, -1, 2, 3, 4, 4, 5, 6, 7, 8, 9)
Y_AT = (2, 3, 4, 5)
BLOCKS = (4, 3, 5, 2, 6, 1, 7, 0)
GROUPS = ((0, 1), (1, 3), (3, 5), (5, 8))


def kernel(f_ref, x_ref, sums, parts_ref, fb, xb, xf, xs, sig, p32, pb, as_, ar, y1s, y1r, y2s, y2r, yb, es, er, bs, br, tot, ys, give,
           s_loc, s_xa, r_xa, r_y, s_x, r_x, s_d, r_d, s_z, r_z, s_a, r_a, s_y1, r_y1, s_y2, r_y2, s_e, s_b, r_b, s_o, s_g, r_o):
    z, c, x = lax.axis_index("z"), lax.axis_index("core"), lax.axis_index("x")
    ylo, yhi = lax.axis_index("ylo"), lax.axis_index("yhi")
    oc, oy, oh = 1 - c, 1 - ylo, 1 - yhi
    xr, xl = lax.rem(x + 1, NX), lax.rem(x + NX - 1, NX)
    zr, zl = lax.rem(z + 1, NZ), lax.rem(z + NZ - 1, NZ)

    partners = [{"z": lax.rem(z + 2, NZ)}, {"z": lax.rem(z + NZ - 2, NZ)}, {"x": xr}, {"x": xl}, {"z": zr}, {"z": zl}, {"core": oc}, {"ylo": oy}, {"ylo": oy, "core": oc},
                {"ylo": oy, "yhi": oh}, {"yhi": oh}]
    barrier = pltpu.get_barrier_semaphore()
    for partner in partners:
        pl.semaphore_signal(barrier, inc=1, device_id=partner, device_id_type=MESH)

    def send(src, dst, ssem, rsem, device):
        copy = pltpu.make_async_remote_copy(
            src_ref=src, dst_ref=dst, send_sem=ssem, recv_sem=rsem, device_id=device, device_id_type=MESH)
        copy.start()

    def landed(ref, rsem, device):
        pltpu.make_async_remote_copy(
            src_ref=ref, dst_ref=ref, send_sem=rsem, recv_sem=rsem, device_id=device, device_id_type=MESH).wait_recv()

    v, vy = 2 * x + ylo, 2 * x + oy
    local = [pltpu.make_async_copy(f_ref.at[4 * ylo + k], fb.at[v, 2 * k], s_loc.at[k]) for k in range(NK)]
    for copy in local:
        copy.start()
    mine = pl.ds(pl.multiple_of(c * 128, 128), 128)
    own_x = pltpu.make_async_copy(x_ref, xf, s_loc.at[NK])
    own_x.start()
    pl.semaphore_wait(barrier, len(partners))

    def place_x(direction, kind, k, at_x):
        if kind == "o":
            return fb.at[2 * at_x + ylo, 2 * k]
        if kind == "y":
            return fb.at[2 * at_x + oy, 2 * k]
        if direction == 0:
            return fb.at[2 * lax.rem(at_x + NX - 1, NX) + ylo, 2 * k]
        return fb.at[2 * lax.rem(at_x + 1, NX) + oy, 2 * k]

    def send_x(direction, n):
        kind, k = (RIGHT, LEFT)[direction][n][0], int((RIGHT, LEFT)[direction][n][1])
        chunk = place_x(direction, kind, k, x)
        send(chunk, chunk, s_x, r_x.at[n], {"x": (xr, xl)[direction]})

    groups = {11: 4, 12: 5}
    parts = {3: [], 4: [], 5: []}

    def across(s, k, n=0):
        group = groups.get(n, k)
        send(fb.at[s, 2 * k], fb.at[s, 2 * k + 1], s_d, r_d.at[group], {"core": oc})
        if k == NK - 1:
            parts[group].append(s)

    def land_x(direction, n):
        kind, k = (RIGHT, LEFT)[direction][n][0], int((RIGHT, LEFT)[direction][n][1])
        sender = (xl, xr)[direction]
        if kind == "o":
            s = 2 * sender + ylo
        elif kind == "y":
            s = 2 * sender + oy
        else:
            s = 2 * lax.rem(x + 2, NX) + (ylo, oy)[direction]
        across(s, k, n + 1)

    def send_z(direction, i):
        if direction == 0:
            chunk = xb.at[lax.rem(z + NZ - i // 2, NZ), i % 2]
        else:
            chunk = xb.at[lax.rem(z + i // 2, NZ), 1 - i % 2]
        send(chunk, chunk, s_z, r_z.at[i], {"z": (zr, zl)[direction]})

    def land_z(i):
        landed(xb.at[0], r_z.at[i], {"z": zl})
        if i < 5:
            send_z(0, i + 2)
            send_z(1, i + 2)

    def tick(n):
        landed(fb.at[0, 0:2], r_x.at[n - 1], {"x": xl})
        land_x(0, n - 1)
        land_x(1, n - 1)
        for k in range(NK):
            if Y_AT[k] == n:
                landed(fb.at[vy, 2 * k], r_y.at[k], {"ylo": oy})
                across(vy, k)
        for m in range(12):
            if RIGHT_AT[m] == n:
                send_x(0, m)
            if LEFT_AT[m] == n:
                send_x(1, m)

    def others_landed(k, group, slices):
        landed(fb.at[0:slices, 2 * k + 1], r_d.at[group], {"core": oc})

    def products(k, slices):
        total = None
        for s in slices:
            part = lax.dot_general(
                fb[s, 2 * k:2 * k + 2].reshape(512, 256), xb[s].reshape(512, 256),
                (((1,), (1,)), ((), ())), preferred_element_type=F32)
            total = part if total is None else total + part
        return total

    def pairs_from(total):
        for q in range(2):
            for m in range(2):
                pb[256 * m:256 * m + 256, 256 * q:256 * q + 256] = (
                    total[256 * q:256 * q + 256, 256 * m:256 * m + 256].astype(BF))

    def near(*steps):
        return [lax.rem(z + n, NZ) for n in steps]

    def mm2_block(k, s):
        part = jnp.dot(pb[...], fb[s, 2 * k:2 * k + 2].reshape(512, 256), preferred_element_type=F32)
        part = part.reshape(2, 2, 128, 256)
        sig[s] = part if k == 0 else sig[s] + part

    def mm2(k):
        for s in range(8):
            mm2_block(k, s)

    for k in range(3):
        local[k].wait()
        send_x(0, k)
        send_x(1, k)
    own_x.wait()
    xs[...] = xf[...].astype(BF)
    xb[z, ylo, :, mine] = xf[c].astype(BF)
    place = xb.at[z, ylo, :, mine]
    send(xs.at[c], place, s_xa, r_xa.at[0], {"ylo": oy})
    send(xs.at[oc], place, s_xa, r_xa.at[1], {"ylo": oy, "core": oc})
    send(xs.at[oc], place, s_xa, r_xa.at[2], {"core": oc})
    for k in range(NK):
        send(f_ref.at[4 * oy + k], fb.at[v, 2 * k], s_x, r_y.at[k], {"ylo": oy})
    local[3].wait()
    for k in range(NK):
        across(v, k)
    landed(xb.at[z, ylo, :, pl.ds(pl.multiple_of(oc * 128, 128), 128)], r_xa.at[2], {"core": oc})
    landed(xb.at[z, oy, :, mine], r_xa.at[0], {"ylo": oy})
    landed(xb.at[z, oy, :, pl.ds(pl.multiple_of(oc * 128, 128), 128)], r_xa.at[1], {"ylo": oy, "core": oc})
    for i in range(2):
        send_z(0, i)
        send_z(1, i)
    for n in range(1, 13):
        tick(n)
        if 3 <= n <= 9:
            land_z(n - 3)
        if n == 7:
            others_landed(0, 0, 8)
            p32[0] = products(0, near(0, 1, 7, 2, 6))
        if n == 8:
            others_landed(1, 1, 8)
            p32[1] = products(1, near(0, 1, 7, 2, 6, 3, 5))
        if n == 9:
            pairs_from(p32[0] + products(0, near(3, 5, 4)))
            mm2(0)
            pairs_from(p32[1] + products(1, near(4)))
        if n == 10:
            mm2(1)
            others_landed(2, 2, 8)
            pairs_from(products(2, range(8)))
        if n == 11:
            mm2(2)
            others_landed(3, 3, 4)
            p32[0] = products(3, parts[3])
            others_landed(3, 4, 2)
            p32[0] += products(3, parts[4])

    def last_pairs(q):
        total = p32[0, 256 * q:256 * q + 256]
        for s in parts[5]:
            total = total + lax.dot_general(
                fb[s, 2 * NK - 2 + q], xb[s].reshape(512, 256), (((1,), (1,)), ((), ())), preferred_element_type=F32)
        for m in range(2):
            pb[256 * m:256 * m + 256, 256 * q:256 * q + 256] = total[:, 256 * m:256 * m + 256].astype(BF)

    def last_block(q, s):
        part = jnp.dot(pb[:, 256 * q:256 * q + 256], fb[s, 2 * NK - 2 + q], preferred_element_type=F32)
        sig[s] = sig[s] + part.reshape(2, 2, 128, 256)

    last_pairs(0)
    for s in near(*BLOCKS):
        last_block(0, s)
    others_landed(3, 5, 2)
    last_pairs(1)

    right = {"ylo": oy, "yhi": lax.rem(yhi + ylo, 2)}
    left = {"ylo": oy, "yhi": lax.rem(yhi + oy, 2)}
    sides = (right, left)
    rings = ({"z": zr}, {"z": zl})
    theirs = pl.ds(pl.multiple_of(oc * 128, 128), 128)

    def block(n):
        return lax.rem(z + BLOCKS[n], NZ)

    def dest(direction, i):
        hops = (4 if i % 2 == 0 else 3) - i // 2
        return BLOCKS.index(hops if direction == 0 else NZ - hops), (i % 2 if direction == 0 else 1 - i % 2)

    halves = (oh, yhi)

    def a_half(i, half):
        if i >= 2:
            landed(ar.at[:, i - 2, half], r_a.at[i - 2, half], rings[1])
        for d in range(2):
            n, slot = dest(d, i)
            own = sig[block(n), slot, halves[half], :, mine]
            if i >= 2:
                own = own + ar[d, i - 2, half].astype(F32)
            as_[d, i, half] = own.astype(BF)
            send(as_.at[d, i, half], ar.at[d, i, half], s_a, r_a.at[i, half], rings[d])

    def a_step(i):
        a_half(i, 0)
        a_half(i, 1)

    kept = []

    def a_last(half):
        for i in (5, 6):
            landed(ar.at[:, i, half], r_a.at[i, half], rings[0])
        for slot in range(2):
            whole = sig[z, slot, halves[half], :, mine] + (
                ar[0, 6 - slot, half].astype(F32) + ar[1, 5 + slot, half].astype(F32))
            if half:
                tot[slot] = whole
                if slot:
                    own = pltpu.make_async_copy(tot.at[ylo], sums.at[c], s_loc.at[0])
                    own.start()
                    kept.append(own)
            ys[slot, half] = whole.astype(BF)
        if half:
            send(ys.at[oy, 1], parts_ref.at[c, 0], s_o, r_o.at[0], {"ylo": oy})
        else:
            send(ys.at[ylo, 0], parts_ref.at[c, 2], s_o, r_o.at[2], {"yhi": oh})
            send(ys.at[oy, 0], parts_ref.at[c, 1], s_o, r_o.at[1], {"ylo": oy, "yhi": oh})

    def far_rows(n, half):
        return sig[block(n), ylo, oh, 64 * half:64 * half + 64, theirs]

    def y1(g):
        lo, hi = GROUPS[g]
        for d in range(2):
            for n in range(lo, hi):
                y1s[d, n] = far_rows(n, d).astype(BF)
            send(y1s.at[d, lo:hi], y1r.at[d, lo:hi], s_y1, r_y1.at[g], sides[d])

    def y2(g):
        lo, hi = GROUPS[g]
        landed(y1r.at[:, lo:hi], r_y1.at[g], sides[1])
        for d in range(2):
            for n in range(lo, hi):
                for half in range(2):
                    own = sig[block(n), sides[d]["ylo"], sides[d]["yhi"], 64 * half:64 * half + 64, theirs]
                    if half == d:
                        own = own + y1r[d, n].astype(F32)
                    y2s[d, n, 64 * half:64 * half + 64] = own.astype(BF)
            send(y2s.at[d, lo:hi], y2r.at[d, lo:hi], s_y2, r_y2.at[g], sides[d])

    def y3(g):
        lo, hi = GROUPS[g]
        landed(y2r.at[:, lo:hi], r_y2.at[g], sides[1])
        for n in range(lo, hi):
            yb[n] = sig[block(n), ylo, yhi, :, theirs] + y2r[0, n].astype(F32) + y2r[1, n].astype(F32)

    two = ({"z": lax.rem(z + 2, NZ)}, {"z": lax.rem(z + NZ - 2, NZ)})

    def b_far():
        for d in range(2):
            es[d] = yb[0, 64 * d:64 * d + 64].astype(BF)
            send(es.at[d], er.at[d], s_e, r_b.at[0], two[d])

    def b_third():
        for d in range(2):
            bs[0, d] = yb[1 + d].astype(BF)
            send(bs.at[0, d], br.at[d], s_b, r_b.at[1], rings[d])

    def b_near():
        for d in range(2):
            bs[1, d] = yb[5 + d].astype(BF)
            send(bs.at[1, d], br.at[2 + d], s_b, r_b.at[2], rings[d])

    def b_second():
        landed(er, r_b.at[0], two[0])
        landed(br.at[0:2], r_b.at[1], rings[0])
        for d in range(2):
            for sub in range(2):
                own = yb[3 + d, 64 * sub:64 * sub + 64] + br[d, 64 * sub:64 * sub + 64].astype(F32)
                if sub == d:
                    own = own + er[d].astype(F32)
                bs[2, d, 64 * sub:64 * sub + 64] = own.astype(BF)
            send(bs.at[2, d], br.at[4 + d], s_b, r_b.at[3], two[d])

    last_block(1, block(0))
    a_step(0)
    y1(0)
    last_block(1, block(1))
    last_block(1, block(2))
    y1(1)
    a_step(1)
    last_block(1, block(3))
    last_block(1, block(4))
    last_block(1, block(5))
    last_block(1, block(6))
    last_block(1, block(7))
    y1(2)
    y1(3)
    y2(0)
    a_half(2, 0)
    y2(1)
    a_half(2, 1)
    a_step(3)
    y2(2)
    a_half(4, 0)
    y3(0)
    b_far()
    a_half(4, 1)
    y2(3)
    y3(1)
    b_third()
    a_step(5)
    y3(2)
    a_half(6, 0)
    a_half(6, 1)
    y3(3)
    b_near()
    b_second()
    a_last(0)
    a_last(1)
    landed(br.at[2:4], r_b.at[2], rings[0])
    give[...] = yb[7] + br[2].astype(F32)
    send(give, sums.at[c], s_g.at[0], r_o.at[3], {"core": oc})
    landed(br.at[4:6], r_b.at[3], two[0])
    send(br.at[3:6], parts_ref.at[c], s_g.at[1], r_o.at[4], {"core": oc})
    kept[0].wait()
    for n, there in enumerate(({"ylo": oy}, {"ylo": oy, "yhi": oh}, {"yhi": oh})):
        landed(parts_ref.at[c, n], r_o.at[n], there)
    landed(sums.at[oc], r_o.at[3], {"core": oc})
    landed(parts_ref.at[oc], r_o.at[4], {"core": oc})
    for ref, sem in ((xb.at[0:3, 0, :, 0:128], s_xa), (fb.at[0:7, 0:4], s_x), (fb.at[0:4], s_d), (xb.at[0:7], s_z), (as_, s_a),
                     (y1s, s_y1), (y2s, s_y2), (es, s_e), (bs, s_b), (br.at[0:3], s_o), (give, s_g.at[0]), (br.at[3:6], s_g.at[1])):
        pltpu.make_async_remote_copy(
            src_ref=ref, dst_ref=ref, send_sem=sem, recv_sem=sem, device_id={"core": oc}, device_id_type=MESH).wait_send()


def per_device(factors, trials):
    dma = pltpu.SemaphoreType.DMA
    sums, parts = pl.pallas_call(
        kernel,
        out_shape=(jax.ShapeDtypeStruct((2, 128, 128), F32), jax.ShapeDtypeStruct((2, 3, 128, 128), BF)),
        in_specs=[pl.BlockSpec(memory_space=pl.ANY), pl.BlockSpec(memory_space=pl.ANY)],
        out_specs=(pl.BlockSpec(memory_space=pl.ANY),) * 2,
        scratch_shapes=[
            pltpu.VMEM((8, 8, 256, 256), BF),
            pltpu.VMEM((8, 2, 256, 256), BF),
            pltpu.VMEM((2, 256, 128), F32),
            pltpu.VMEM((2, 256, 128), BF),
            pltpu.VMEM((8, 2, 2, 128, 256), F32),
            pltpu.VMEM((2, 512, 512), F32),
            pltpu.VMEM((512, 512), BF),
            pltpu.VMEM((2, 7, 2, 128, 128), BF),
            pltpu.VMEM((2, 7, 2, 128, 128), BF),
            pltpu.VMEM((2, 8, 64, 128), BF),
            pltpu.VMEM((2, 8, 64, 128), BF),
            pltpu.VMEM((2, 8, 128, 128), BF),
            pltpu.VMEM((2, 8, 128, 128), BF),
            pltpu.VMEM((8, 128, 128), F32),
            pltpu.VMEM((2, 64, 128), BF),
            pltpu.VMEM((2, 64, 128), BF),
            pltpu.VMEM((3, 2, 128, 128), BF),
            pltpu.VMEM((6, 128, 128), BF),
            pltpu.VMEM((2, 128, 128), F32),
            pltpu.VMEM((2, 2, 128, 128), BF),
            pltpu.VMEM((128, 128), F32),
            dma((5,)), dma(()), dma((3,)), dma((4,)), dma(()), dma((12,)),
            dma(()), dma((6,)), dma(()), dma((7,)), dma(()), dma((7, 2)),
            dma(()), dma((4,)), dma(()), dma((4,)), dma(()), dma(()), dma((4,)), dma(()), dma((2,)), dma((5,)),
        ],
        compiler_params=pltpu.CompilerParams(
            collective_id=0, has_side_effects=True, vmem_limit_bytes=60000 * 1024),
    )(factors, trials)
    far, side, near = (parts[:, n].astype(F32) for n in range(3))
    return (sums + far) + (side + near)


def solution(mesh):
    torus = Mesh(mesh.devices.reshape(NZ, 2, NX, 2, 2), ("z", "core", "x", "ylo", "yhi"))
    in_specs = (P(("z", "core", "yhi"), None, ("x", "ylo")), P(("x", "ylo"), None, ("z", "core")))
    out_specs = P(("x", "ylo"), "yhi", ("z", "core"))
    return jax.shard_map(
        per_device, mesh=torus, in_specs=in_specs, out_specs=out_specs, check_vma=False
    )
```

```python
import jax
import jax.numpy as jnp
from jax import lax
from jax.experimental import pallas as pl
from jax.experimental.pallas import tpu as pltpu
from jax.sharding import Mesh
from jax.sharding import PartitionSpec as P

MESH = pl.DeviceIdType.MESH
BF, F32 = jnp.bfloat16, jnp.float32
NX, NZ, NK = 4, 8, 4
RIGHT = ("o0", "o1", "o2", "f0", "f1", "y0", "f2", "y1", "o3", "y2", "f3", "y3")
LEFT = ("o0", "o1", "o2", "y0", "y1", "f0", "y2", "f1", "y3", "f2", "o3", "f3")
RIGHT_AT = (-1, -1, -1, 1, 2, 3, 4, 5, 6, 7, 9, 9)
LEFT_AT = (-1, -1, -1, 2, 3, 4, 4, 5, 6, 7, 8, 9)
Y_AT = (2, 3, 4, 5)
BLOCKS = (4, 3, 5, 2, 6, 1, 7, 0)
GROUPS = ((0, 1), (1, 3), (3, 5), (5, 8))


def kernel(f_ref, x_ref, sums, parts_ref, fb, xb, xf, xs, sig, p32, pb, as_, ar, y1s, y1r, y2s, y2r, yb, es, er, bs, br, tot, ys, none,
           s_loc, s_xa, r_xa, r_y, s_x, r_x, s_d, r_d, s_z, r_z, s_a, r_a, s_y1, r_y1, s_y2, r_y2, s_e, s_b, r_b, s_o, s_g, r_o):
    z, c, x = lax.axis_index("z"), lax.axis_index("core"), lax.axis_index("x")
    ylo, yhi = lax.axis_index("ylo"), lax.axis_index("yhi")
    oc, oy, oh = 1 - c, 1 - ylo, 1 - yhi
    xr, xl = lax.rem(x + 1, NX), lax.rem(x + NX - 1, NX)
    zr, zl = lax.rem(z + 1, NZ), lax.rem(z + NZ - 1, NZ)

    partners = [{"z": lax.rem(z + n, NZ), "core": oc} for n in (1, 2, NZ - 2, NZ - 1)]
    partners += [{"z": lax.rem(z + 2, NZ)}, {"z": lax.rem(z + NZ - 2, NZ)}, {"x": xr}, {"x": xl}, {"z": zr}, {"z": zl}, {"core": oc}, {"ylo": oy}, {"ylo": oy, "core": oc},
                {"ylo": oy, "yhi": oh}, {"yhi": oh}]
    barrier = pltpu.get_barrier_semaphore()
    for partner in partners:
        pl.semaphore_signal(barrier, inc=1, device_id=partner, device_id_type=MESH)

    def send(src, dst, ssem, rsem, device):
        copy = pltpu.make_async_remote_copy(
            src_ref=src, dst_ref=dst, send_sem=ssem, recv_sem=rsem, device_id=device, device_id_type=MESH)
        copy.start()

    def landed(ref, rsem, device):
        pltpu.make_async_remote_copy(
            src_ref=ref, dst_ref=ref, send_sem=rsem, recv_sem=rsem, device_id=device, device_id_type=MESH).wait_recv()

    v, vy = 2 * x + ylo, 2 * x + oy
    local = [pltpu.make_async_copy(f_ref.at[4 * ylo + k], fb.at[v, 2 * k], s_loc.at[k]) for k in range(NK)]
    for copy in local:
        copy.start()
    mine = pl.ds(pl.multiple_of(c * 128, 128), 128)
    own_x = pltpu.make_async_copy(x_ref, xf, s_loc.at[NK])
    own_x.start()
    pl.semaphore_wait(barrier, len(partners))

    def place_x(direction, kind, k, at_x):
        if kind == "o":
            return fb.at[2 * at_x + ylo, 2 * k]
        if kind == "y":
            return fb.at[2 * at_x + oy, 2 * k]
        if direction == 0:
            return fb.at[2 * lax.rem(at_x + NX - 1, NX) + ylo, 2 * k]
        return fb.at[2 * lax.rem(at_x + 1, NX) + oy, 2 * k]

    def send_x(direction, n):
        kind, k = (RIGHT, LEFT)[direction][n][0], int((RIGHT, LEFT)[direction][n][1])
        chunk = place_x(direction, kind, k, x)
        send(chunk, chunk, s_x, r_x.at[n], {"x": (xr, xl)[direction]})

    groups = {11: 4, 12: 5}
    parts = {3: [], 4: [], 5: []}

    def across(s, k, n=0):
        group = groups.get(n, k)
        send(fb.at[s, 2 * k], fb.at[s, 2 * k + 1], s_d, r_d.at[group], {"core": oc})
        if k == NK - 1:
            parts[group].append(s)

    def land_x(direction, n):
        kind, k = (RIGHT, LEFT)[direction][n][0], int((RIGHT, LEFT)[direction][n][1])
        sender = (xl, xr)[direction]
        if kind == "o":
            s = 2 * sender + ylo
        elif kind == "y":
            s = 2 * sender + oy
        else:
            s = 2 * lax.rem(x + 2, NX) + (ylo, oy)[direction]
        across(s, k, n + 1)

    def send_z(direction, i):
        if direction == 0:
            chunk = xb.at[lax.rem(z + NZ - i // 2, NZ), i % 2]
        else:
            chunk = xb.at[lax.rem(z + i // 2, NZ), 1 - i % 2]
        send(chunk, chunk, s_z, r_z.at[i], {"z": (zr, zl)[direction]})

    def land_z(i):
        landed(xb.at[0], r_z.at[i], {"z": zl})
        if i < 5:
            send_z(0, i + 2)
            send_z(1, i + 2)

    def tick(n):
        landed(fb.at[0, 0:2], r_x.at[n - 1], {"x": xl})
        land_x(0, n - 1)
        land_x(1, n - 1)
        for k in range(NK):
            if Y_AT[k] == n:
                landed(fb.at[vy, 2 * k], r_y.at[k], {"ylo": oy})
                across(vy, k)
        for m in range(12):
            if RIGHT_AT[m] == n:
                send_x(0, m)
            if LEFT_AT[m] == n:
                send_x(1, m)

    def others_landed(k, group, slices):
        landed(fb.at[0:slices, 2 * k + 1], r_d.at[group], {"core": oc})

    def products(k, slices):
        total = None
        for s in slices:
            part = lax.dot_general(
                fb[s, 2 * k:2 * k + 2].reshape(512, 256), xb[s].reshape(512, 256),
                (((1,), (1,)), ((), ())), preferred_element_type=F32)
            total = part if total is None else total + part
        return total

    def pairs_from(total):
        for q in range(2):
            for m in range(2):
                pb[256 * m:256 * m + 256, 256 * q:256 * q + 256] = (
                    total[256 * q:256 * q + 256, 256 * m:256 * m + 256].astype(BF))

    def near(*steps):
        return [lax.rem(z + n, NZ) for n in steps]

    def mm2_block(k, s):
        part = jnp.dot(pb[...], fb[s, 2 * k:2 * k + 2].reshape(512, 256), preferred_element_type=F32)
        part = part.reshape(2, 2, 128, 256)
        sig[s] = part if k == 0 else sig[s] + part

    def mm2(k):
        for s in range(8):
            mm2_block(k, s)

    for k in range(3):
        local[k].wait()
        send_x(0, k)
        send_x(1, k)
    none[...] = jnp.zeros_like(none)
    blank = pltpu.make_async_copy(none, parts_ref.at[c, 3], s_loc.at[1])
    own_x.wait()
    blank.start()
    xs[...] = xf[...].astype(BF)
    xb[z, ylo, :, mine] = xf[c].astype(BF)
    place = xb.at[z, ylo, :, mine]
    send(xs.at[c], place, s_xa, r_xa.at[0], {"ylo": oy})
    send(xs.at[oc], place, s_xa, r_xa.at[1], {"ylo": oy, "core": oc})
    send(xs.at[oc], place, s_xa, r_xa.at[2], {"core": oc})
    for k in range(NK):
        send(f_ref.at[4 * oy + k], fb.at[v, 2 * k], s_x, r_y.at[k], {"ylo": oy})
    local[3].wait()
    for k in range(NK):
        across(v, k)
    landed(xb.at[z, ylo, :, pl.ds(pl.multiple_of(oc * 128, 128), 128)], r_xa.at[2], {"core": oc})
    landed(xb.at[z, oy, :, mine], r_xa.at[0], {"ylo": oy})
    landed(xb.at[z, oy, :, pl.ds(pl.multiple_of(oc * 128, 128), 128)], r_xa.at[1], {"ylo": oy, "core": oc})
    for i in range(2):
        send_z(0, i)
        send_z(1, i)
    for n in range(1, 13):
        tick(n)
        if 3 <= n <= 9:
            land_z(n - 3)
        if n == 7:
            others_landed(0, 0, 8)
            p32[0] = products(0, near(0, 1, 7, 2, 6))
        if n == 8:
            others_landed(1, 1, 8)
            p32[1] = products(1, near(0, 1, 7, 2, 6, 3, 5))
        if n == 9:
            pairs_from(p32[0] + products(0, near(3, 5, 4)))
            mm2(0)
            pairs_from(p32[1] + products(1, near(4)))
        if n == 10:
            mm2(1)
            others_landed(2, 2, 8)
            pairs_from(products(2, range(8)))
        if n == 11:
            mm2(2)
            others_landed(3, 3, 4)
            p32[0] = products(3, parts[3])
            others_landed(3, 4, 2)
            p32[0] += products(3, parts[4])

    def last_pairs(q):
        total = p32[0, 256 * q:256 * q + 256]
        for s in parts[5]:
            total = total + lax.dot_general(
                fb[s, 2 * NK - 2 + q], xb[s].reshape(512, 256), (((1,), (1,)), ((), ())), preferred_element_type=F32)
        for m in range(2):
            pb[256 * m:256 * m + 256, 256 * q:256 * q + 256] = total[:, 256 * m:256 * m + 256].astype(BF)

    def last_block(q, s):
        part = jnp.dot(pb[:, 256 * q:256 * q + 256], fb[s, 2 * NK - 2 + q], preferred_element_type=F32)
        sig[s] = sig[s] + part.reshape(2, 2, 128, 256)

    last_pairs(0)
    for s in near(*BLOCKS):
        last_block(0, s)
    others_landed(3, 5, 2)
    last_pairs(1)

    right = {"ylo": oy, "yhi": lax.rem(yhi + ylo, 2)}
    left = {"ylo": oy, "yhi": lax.rem(yhi + oy, 2)}
    sides = (right, left)
    rings = ({"z": zr}, {"z": zl})
    theirs = pl.ds(pl.multiple_of(oc * 128, 128), 128)

    def block(n):
        return lax.rem(z + BLOCKS[n], NZ)

    def dest(direction, i):
        hops = (4 if i % 2 == 0 else 3) - i // 2
        return BLOCKS.index(hops if direction == 0 else NZ - hops), (i % 2 if direction == 0 else 1 - i % 2)

    halves = (oh, yhi)

    def a_half(i, half):
        if i >= 2:
            landed(ar.at[:, i - 2, half], r_a.at[i - 2, half], rings[1])
        for d in range(2):
            n, slot = dest(d, i)
            own = sig[block(n), slot, halves[half], :, mine]
            if i >= 2:
                own = own + ar[d, i - 2, half].astype(F32)
            as_[d, i, half] = own.astype(BF)
            send(as_.at[d, i, half], ar.at[d, i, half], s_a, r_a.at[i, half], rings[d])

    def a_step(i):
        a_half(i, 0)
        a_half(i, 1)

    kept = []

    def a_last(half):
        for i in (5, 6):
            landed(ar.at[:, i, half], r_a.at[i, half], rings[0])
        for slot in range(2):
            whole = sig[z, slot, halves[half], :, mine] + (
                ar[0, 6 - slot, half].astype(F32) + ar[1, 5 + slot, half].astype(F32))
            if half:
                tot[slot] = whole
                if slot:
                    own = pltpu.make_async_copy(tot.at[ylo], sums.at[c], s_loc.at[0])
                    own.start()
                    kept.append(own)
            ys[slot, half] = whole.astype(BF)
        if half:
            send(ys.at[oy, 1], parts_ref.at[c, 0], s_o, r_o.at[0], {"ylo": oy})
        else:
            send(ys.at[ylo, 0], parts_ref.at[c, 2], s_o, r_o.at[2], {"yhi": oh})
            send(ys.at[oy, 0], parts_ref.at[c, 1], s_o, r_o.at[1], {"ylo": oy, "yhi": oh})

    def far_rows(n, half):
        return sig[block(n), ylo, oh, 64 * half:64 * half + 64, theirs]

    def y1(g):
        lo, hi = GROUPS[g]
        for d in range(2):
            for n in range(lo, hi):
                y1s[d, n] = far_rows(n, d).astype(BF)
            send(y1s.at[d, lo:hi], y1r.at[d, lo:hi], s_y1, r_y1.at[g], sides[d])

    def y2(g):
        lo, hi = GROUPS[g]
        landed(y1r.at[:, lo:hi], r_y1.at[g], sides[1])
        for d in range(2):
            for n in range(lo, hi):
                for half in range(2):
                    own = sig[block(n), sides[d]["ylo"], sides[d]["yhi"], 64 * half:64 * half + 64, theirs]
                    if half == d:
                        own = own + y1r[d, n].astype(F32)
                    y2s[d, n, 64 * half:64 * half + 64] = own.astype(BF)
            send(y2s.at[d, lo:hi], y2r.at[d, lo:hi], s_y2, r_y2.at[g], sides[d])

    def y3(g):
        lo, hi = GROUPS[g]
        landed(y2r.at[:, lo:hi], r_y2.at[g], sides[1])
        for n in range(lo, hi):
            yb[n] = sig[block(n), ylo, yhi, :, theirs] + y2r[0, n].astype(F32) + y2r[1, n].astype(F32)

    two = ({"z": lax.rem(z + 2, NZ)}, {"z": lax.rem(z + NZ - 2, NZ)})

    def b_far():
        for d in range(2):
            es[d] = yb[0, 64 * d:64 * d + 64].astype(BF)
            send(es.at[d], er.at[d], s_e, r_b.at[0], two[d])

    def b_third():
        for d in range(2):
            bs[0, d] = yb[1 + d].astype(BF)
            send(bs.at[0, d], br.at[d], s_b, r_b.at[1], rings[d])

    def b_near():
        for d in range(2):
            bs[1, d] = yb[5 + d].astype(BF)
            send(bs.at[1, d], parts_ref.at[c, d], s_b, r_b.at[2], rings[d] | {"core": oc})
        send(yb.at[7], sums.at[c], s_g, r_o.at[3], {"core": oc})

    def b_second():
        landed(er, r_b.at[0], two[0])
        landed(br, r_b.at[1], rings[0])
        for d in range(2):
            for sub in range(2):
                own = yb[3 + d, 64 * sub:64 * sub + 64] + br[d, 64 * sub:64 * sub + 64].astype(F32)
                if sub == d:
                    own = own + er[d].astype(F32)
                bs[2, d, 64 * sub:64 * sub + 64] = own.astype(BF)
            send(bs.at[2, d], parts_ref.at[c, 2 + d], s_b, r_b.at[3], two[d] | {"core": oc})

    last_block(1, block(0))
    a_step(0)
    y1(0)
    last_block(1, block(1))
    last_block(1, block(2))
    a_step(1)
    y1(1)
    last_block(1, block(3))
    last_block(1, block(4))
    last_block(1, block(5))
    last_block(1, block(6))
    last_block(1, block(7))
    y1(2)
    y1(3)
    y2(0)
    a_half(2, 0)
    a_half(2, 1)
    y2(1)
    a_step(3)
    y2(2)
    a_half(4, 0)
    a_half(4, 1)
    y3(0)
    b_far()
    y2(3)
    y3(1)
    b_third()
    a_step(5)
    a_half(6, 0)
    y3(2)
    a_half(6, 1)
    b_second()
    y3(3)
    b_near()
    a_last(0)
    a_last(1)
    blank.wait()
    kept[0].wait()
    landed(sums.at[oc], r_o.at[3], {"core": oc})
    landed(parts_ref.at[oc, 0:2], r_b.at[2], rings[0])
    landed(parts_ref.at[oc, 2:4], r_b.at[3], two[0])
    for n, there in enumerate(({"ylo": oy}, {"ylo": oy, "yhi": oh}, {"yhi": oh})):
        landed(parts_ref.at[c, n], r_o.at[n], there)
    for ref, sem in ((xb.at[0:3, 0, :, 0:128], s_xa), (fb.at[0:7, 0:4], s_x), (fb.at[0:4], s_d), (xb.at[0:7], s_z), (as_, s_a),
                     (y1s, s_y1), (y2s, s_y2), (es, s_e), (bs, s_b), (y2r.at[0, 0:3], s_o), (yb.at[7], s_g)):
        pltpu.make_async_remote_copy(
            src_ref=ref, dst_ref=ref, send_sem=sem, recv_sem=sem, device_id={"core": oc}, device_id_type=MESH).wait_send()


def per_device(factors, trials):
    dma = pltpu.SemaphoreType.DMA
    sums, parts = pl.pallas_call(
        kernel,
        out_shape=(jax.ShapeDtypeStruct((2, 128, 128), F32), jax.ShapeDtypeStruct((2, 4, 128, 128), BF)),
        in_specs=[pl.BlockSpec(memory_space=pl.ANY), pl.BlockSpec(memory_space=pl.ANY)],
        out_specs=(pl.BlockSpec(memory_space=pl.ANY),) * 2,
        scratch_shapes=[
            pltpu.VMEM((8, 8, 256, 256), BF),
            pltpu.VMEM((8, 2, 256, 256), BF),
            pltpu.VMEM((2, 256, 128), F32),
            pltpu.VMEM((2, 256, 128), BF),
            pltpu.VMEM((8, 2, 2, 128, 256), F32),
            pltpu.VMEM((2, 512, 512), F32),
            pltpu.VMEM((512, 512), BF),
            pltpu.VMEM((2, 7, 2, 128, 128), BF),
            pltpu.VMEM((2, 7, 2, 128, 128), BF),
            pltpu.VMEM((2, 8, 64, 128), BF),
            pltpu.VMEM((2, 8, 64, 128), BF),
            pltpu.VMEM((2, 8, 128, 128), BF),
            pltpu.VMEM((2, 8, 128, 128), BF),
            pltpu.VMEM((8, 128, 128), F32),
            pltpu.VMEM((2, 64, 128), BF),
            pltpu.VMEM((2, 64, 128), BF),
            pltpu.VMEM((3, 2, 128, 128), BF),
            pltpu.VMEM((2, 128, 128), BF),
            pltpu.VMEM((2, 128, 128), F32),
            pltpu.VMEM((2, 2, 128, 128), BF),
            pltpu.VMEM((128, 128), BF),
            dma((5,)), dma(()), dma((3,)), dma((4,)), dma(()), dma((12,)),
            dma(()), dma((6,)), dma(()), dma((7,)), dma(()), dma((7, 2)),
            dma(()), dma((4,)), dma(()), dma((4,)), dma(()), dma(()), dma((4,)), dma(()), dma(()), dma((4,)),
        ],
        compiler_params=pltpu.CompilerParams(
            collective_id=0, has_side_effects=True, vmem_limit_bytes=60000 * 1024),
    )(factors, trials)
    a, b, c, d = (parts[:, n].astype(F32) for n in range(4))
    return (sums + a) + (b + (c + d))


def solution(mesh):
    torus = Mesh(mesh.devices.reshape(NZ, 2, NX, 2, 2), ("z", "core", "x", "ylo", "yhi"))
    in_specs = (P(("z", "core", "yhi"), None, ("x", "ylo")), P(("x", "ylo"), None, ("z", "core")))
    out_specs = P(("x", "ylo"), "yhi", ("z", "core"))
    return jax.shard_map(
        per_device, mesh=torus, in_specs=in_specs, out_specs=out_specs, check_vma=False
    )
```

```python
import jax
import jax.numpy as jnp
from jax import lax
from jax.experimental import pallas as pl
from jax.experimental.pallas import tpu as pltpu
from jax.sharding import Mesh
from jax.sharding import PartitionSpec as P

MESH = pl.DeviceIdType.MESH
BF, F32 = jnp.bfloat16, jnp.float32
NX, NZ, NK = 4, 8, 4
RIGHT = ("o0", "o1", "o2", "f0", "f1", "y0", "f2", "y1", "o3", "y2", "f3", "y3")
LEFT = ("o0", "o1", "o2", "y0", "y1", "f0", "y2", "f1", "y3", "f2", "o3", "f3")
RIGHT_AT = (-1, -1, -1, 1, 2, 3, 4, 5, 6, 7, 9, 9)
LEFT_AT = (-1, -1, -1, 2, 3, 4, 4, 5, 6, 7, 8, 9)
Y_AT = (2, 3, 4, 5)
BLOCKS = (4, 3, 5, 2, 6, 1, 7, 0)
GROUPS = ((0, 1), (1, 3), (3, 5), (5, 8))


def kernel(f_ref, x_ref, sums, parts_ref, fb, xb, xf, xs, sig, p32, pb, as_, ar, y1s, y1r, y2s, y2r, yb, es, er, bs, br, tot, ys, none,
           s_loc, s_xa, r_xa, r_y, s_x, r_x, s_d, r_d, s_z, r_z, s_a, r_a, s_y1, r_y1, s_y2, r_y2, s_e, s_b, r_b, s_o, s_g, r_o):
    z, c, x = lax.axis_index("z"), lax.axis_index("core"), lax.axis_index("x")
    ylo, yhi = lax.axis_index("ylo"), lax.axis_index("yhi")
    oc, oy, oh = 1 - c, 1 - ylo, 1 - yhi
    xr, xl = lax.rem(x + 1, NX), lax.rem(x + NX - 1, NX)
    zr, zl = lax.rem(z + 1, NZ), lax.rem(z + NZ - 1, NZ)

    partners = [{"z": lax.rem(z + n, NZ), "core": oc} for n in (1, 2, NZ - 2, NZ - 1)]
    partners += [{"z": lax.rem(z + 2, NZ)}, {"z": lax.rem(z + NZ - 2, NZ)}, {"x": xr}, {"x": xl}, {"z": zr}, {"z": zl}, {"core": oc}, {"ylo": oy}, {"ylo": oy, "core": oc},
                {"ylo": oy, "yhi": oh}, {"yhi": oh}]
    barrier = pltpu.get_barrier_semaphore()
    for partner in partners:
        pl.semaphore_signal(barrier, inc=1, device_id=partner, device_id_type=MESH)

    def send(src, dst, ssem, rsem, device):
        copy = pltpu.make_async_remote_copy(
            src_ref=src, dst_ref=dst, send_sem=ssem, recv_sem=rsem, device_id=device, device_id_type=MESH)
        copy.start()

    def landed(ref, rsem, device):
        pltpu.make_async_remote_copy(
            src_ref=ref, dst_ref=ref, send_sem=rsem, recv_sem=rsem, device_id=device, device_id_type=MESH).wait_recv()

    v, vy = 2 * x + ylo, 2 * x + oy
    local = [pltpu.make_async_copy(f_ref.at[4 * ylo + k], fb.at[v, 2 * k], s_loc.at[k]) for k in range(NK)]
    for copy in local:
        copy.start()
    mine = pl.ds(pl.multiple_of(c * 128, 128), 128)
    own_x = pltpu.make_async_copy(x_ref, xf, s_loc.at[NK])
    own_x.start()
    pl.semaphore_wait(barrier, len(partners))

    def place_x(direction, kind, k, at_x):
        if kind == "o":
            return fb.at[2 * at_x + ylo, 2 * k]
        if kind == "y":
            return fb.at[2 * at_x + oy, 2 * k]
        if direction == 0:
            return fb.at[2 * lax.rem(at_x + NX - 1, NX) + ylo, 2 * k]
        return fb.at[2 * lax.rem(at_x + 1, NX) + oy, 2 * k]

    def send_x(direction, n):
        kind, k = (RIGHT, LEFT)[direction][n][0], int((RIGHT, LEFT)[direction][n][1])
        chunk = place_x(direction, kind, k, x)
        send(chunk, chunk, s_x, r_x.at[n], {"x": (xr, xl)[direction]})

    groups = {11: 4, 12: 5}
    parts = {3: [], 4: [], 5: []}

    def across(s, k, n=0):
        group = groups.get(n, k)
        send(fb.at[s, 2 * k], fb.at[s, 2 * k + 1], s_d, r_d.at[group], {"core": oc})
        if k == NK - 1:
            parts[group].append(s)

    def land_x(direction, n):
        kind, k = (RIGHT, LEFT)[direction][n][0], int((RIGHT, LEFT)[direction][n][1])
        sender = (xl, xr)[direction]
        if kind == "o":
            s = 2 * sender + ylo
        elif kind == "y":
            s = 2 * sender + oy
        else:
            s = 2 * lax.rem(x + 2, NX) + (ylo, oy)[direction]
        across(s, k, n + 1)

    def send_z(direction, i):
        if direction == 0:
            chunk = xb.at[lax.rem(z + NZ - i // 2, NZ), i % 2]
        else:
            chunk = xb.at[lax.rem(z + i // 2, NZ), 1 - i % 2]
        send(chunk, chunk, s_z, r_z.at[i], {"z": (zr, zl)[direction]})

    def land_z(i):
        landed(xb.at[0], r_z.at[i], {"z": zl})
        if i < 5:
            send_z(0, i + 2)
            send_z(1, i + 2)

    def tick(n):
        landed(fb.at[0, 0:2], r_x.at[n - 1], {"x": xl})
        land_x(0, n - 1)
        land_x(1, n - 1)
        for k in range(NK):
            if Y_AT[k] == n:
                landed(fb.at[vy, 2 * k], r_y.at[k], {"ylo": oy})
                across(vy, k)
        for m in range(12):
            if RIGHT_AT[m] == n:
                send_x(0, m)
            if LEFT_AT[m] == n:
                send_x(1, m)

    def others_landed(k, group, slices):
        landed(fb.at[0:slices, 2 * k + 1], r_d.at[group], {"core": oc})

    def products(k, slices):
        total = None
        for s in slices:
            part = lax.dot_general(
                fb[s, 2 * k:2 * k + 2].reshape(512, 256), xb[s].reshape(512, 256),
                (((1,), (1,)), ((), ())), preferred_element_type=F32)
            total = part if total is None else total + part
        return total

    def pairs_from(total):
        for q in range(2):
            for m in range(2):
                pb[256 * m:256 * m + 256, 256 * q:256 * q + 256] = (
                    total[256 * q:256 * q + 256, 256 * m:256 * m + 256].astype(BF))

    def near(*steps):
        return [lax.rem(z + n, NZ) for n in steps]

    def mm2_block(k, s):
        part = jnp.dot(pb[...], fb[s, 2 * k:2 * k + 2].reshape(512, 256), preferred_element_type=F32)
        part = part.reshape(2, 2, 128, 256)
        sig[s] = part if k == 0 else sig[s] + part

    def mm2(k):
        for s in range(8):
            mm2_block(k, s)

    for k in range(3):
        local[k].wait()
        send_x(0, k)
        send_x(1, k)
    none[...] = jnp.zeros_like(none)
    blank = pltpu.make_async_copy(none, parts_ref.at[c, 3], s_loc.at[1])
    own_x.wait()
    blank.start()
    xs[...] = xf[...].astype(BF)
    xb[z, ylo, :, mine] = xf[c].astype(BF)
    place = xb.at[z, ylo, :, mine]
    send(xs.at[c], place, s_xa, r_xa.at[0], {"ylo": oy})
    send(xs.at[oc], place, s_xa, r_xa.at[1], {"ylo": oy, "core": oc})
    send(xs.at[oc], place, s_xa, r_xa.at[2], {"core": oc})
    for k in range(NK):
        send(f_ref.at[4 * oy + k], fb.at[v, 2 * k], s_x, r_y.at[k], {"ylo": oy})
    local[3].wait()
    for k in range(NK):
        across(v, k)
    landed(xb.at[z, ylo, :, pl.ds(pl.multiple_of(oc * 128, 128), 128)], r_xa.at[2], {"core": oc})
    landed(xb.at[z, oy, :, mine], r_xa.at[0], {"ylo": oy})
    landed(xb.at[z, oy, :, pl.ds(pl.multiple_of(oc * 128, 128), 128)], r_xa.at[1], {"ylo": oy, "core": oc})
    for i in range(2):
        send_z(0, i)
        send_z(1, i)
    for n in range(1, 13):
        tick(n)
        if 3 <= n <= 9:
            land_z(n - 3)
        if n == 7:
            others_landed(0, 0, 8)
            p32[0] = products(0, near(0, 1, 7, 2, 6))
        if n == 8:
            others_landed(1, 1, 8)
            p32[1] = products(1, near(0, 1, 7, 2, 6, 3, 5))
        if n == 9:
            pairs_from(p32[0] + products(0, near(3, 5, 4)))
            mm2(0)
            pairs_from(p32[1] + products(1, near(4)))
        if n == 10:
            mm2(1)
            others_landed(2, 2, 8)
            pairs_from(products(2, range(8)))
        if n == 11:
            mm2(2)
            others_landed(3, 3, 4)
            p32[0] = products(3, parts[3])
            others_landed(3, 4, 2)
            p32[0] += products(3, parts[4])

    def last_pairs(q):
        total = p32[0, 256 * q:256 * q + 256]
        for s in parts[5]:
            total = total + lax.dot_general(
                fb[s, 2 * NK - 2 + q], xb[s].reshape(512, 256), (((1,), (1,)), ((), ())), preferred_element_type=F32)
        for m in range(2):
            pb[256 * m:256 * m + 256, 256 * q:256 * q + 256] = total[:, 256 * m:256 * m + 256].astype(BF)

    def last_block(q, s):
        part = jnp.dot(pb[:, 256 * q:256 * q + 256], fb[s, 2 * NK - 2 + q], preferred_element_type=F32)
        sig[s] = sig[s] + part.reshape(2, 2, 128, 256)

    def last_blocks(q, slices):
        parts_of = [jnp.dot(pb[:, 256 * q:256 * q + 256], fb[s, 2 * NK - 2 + q], preferred_element_type=F32) for s in slices]
        for s, part in zip(slices, parts_of):
            sig[s] = sig[s] + part.reshape(2, 2, 128, 256)

    last_pairs(0)
    for s in near(*BLOCKS):
        last_block(0, s)
    others_landed(3, 5, 2)
    last_pairs(1)

    right = {"ylo": oy, "yhi": lax.rem(yhi + ylo, 2)}
    left = {"ylo": oy, "yhi": lax.rem(yhi + oy, 2)}
    sides = (right, left)
    rings = ({"z": zr}, {"z": zl})
    theirs = pl.ds(pl.multiple_of(oc * 128, 128), 128)

    def block(n):
        return lax.rem(z + BLOCKS[n], NZ)

    def dest(direction, i):
        hops = (4 if i % 2 == 0 else 3) - i // 2
        return BLOCKS.index(hops if direction == 0 else NZ - hops), (i % 2 if direction == 0 else 1 - i % 2)

    halves = (oh, yhi)

    def a_half(i, half):
        if i >= 2:
            landed(ar.at[:, i - 2, half], r_a.at[i - 2, half], rings[1])
        for d in range(2):
            n, slot = dest(d, i)
            own = sig[block(n), slot, halves[half], :, mine]
            if i >= 2:
                own = own + ar[d, i - 2, half].astype(F32)
            as_[d, i, half] = own.astype(BF)
            send(as_.at[d, i, half], ar.at[d, i, half], s_a, r_a.at[i, half], rings[d])

    def a_step(i):
        a_half(i, 0)
        a_half(i, 1)

    kept = []

    def a_last(half):
        for i in (5, 6):
            landed(ar.at[:, i, half], r_a.at[i, half], rings[0])
        for slot in range(2):
            whole = sig[z, slot, halves[half], :, mine] + (
                ar[0, 6 - slot, half].astype(F32) + ar[1, 5 + slot, half].astype(F32))
            if half:
                tot[slot] = whole
                if slot:
                    own = pltpu.make_async_copy(tot.at[ylo], sums.at[c], s_loc.at[0])
                    own.start()
                    kept.append(own)
            ys[slot, half] = whole.astype(BF)
        if half:
            send(ys.at[oy, 1], parts_ref.at[c, 0], s_o, r_o.at[0], {"ylo": oy})
        else:
            send(ys.at[ylo, 0], parts_ref.at[c, 2], s_o, r_o.at[2], {"yhi": oh})
            send(ys.at[oy, 0], parts_ref.at[c, 1], s_o, r_o.at[1], {"ylo": oy, "yhi": oh})

    def far_rows(n, half):
        return sig[block(n), ylo, oh, 64 * half:64 * half + 64, theirs]

    def y1(g):
        lo, hi = GROUPS[g]
        for d in range(2):
            for n in range(lo, hi):
                y1s[d, n] = far_rows(n, d).astype(BF)
            send(y1s.at[d, lo:hi], y1r.at[d, lo:hi], s_y1, r_y1.at[g], sides[d])

    def y2(g):
        lo, hi = GROUPS[g]
        landed(y1r.at[:, lo:hi], r_y1.at[g], sides[1])
        for d in range(2):
            for n in range(lo, hi):
                for half in range(2):
                    own = sig[block(n), sides[d]["ylo"], sides[d]["yhi"], 64 * half:64 * half + 64, theirs]
                    if half == d:
                        own = own + y1r[d, n].astype(F32)
                    y2s[d, n, 64 * half:64 * half + 64] = own.astype(BF)
            send(y2s.at[d, lo:hi], y2r.at[d, lo:hi], s_y2, r_y2.at[g], sides[d])

    def y3(g):
        lo, hi = GROUPS[g]
        landed(y2r.at[:, lo:hi], r_y2.at[g], sides[1])
        for n in range(lo, hi):
            yb[n] = sig[block(n), ylo, yhi, :, theirs] + y2r[0, n].astype(F32) + y2r[1, n].astype(F32)

    two = ({"z": lax.rem(z + 2, NZ)}, {"z": lax.rem(z + NZ - 2, NZ)})

    def b_far():
        for d in range(2):
            es[d] = yb[0, 64 * d:64 * d + 64].astype(BF)
            send(es.at[d], er.at[d], s_e, r_b.at[0], two[d])

    def b_third():
        for d in range(2):
            bs[0, d] = yb[1 + d].astype(BF)
            send(bs.at[0, d], br.at[d], s_b, r_b.at[1], rings[d])

    def b_near():
        for d in range(2):
            bs[1, d] = yb[5 + d].astype(BF)
            send(bs.at[1, d], parts_ref.at[c, d], s_b, r_b.at[2], rings[d] | {"core": oc})
        send(yb.at[7], sums.at[c], s_g, r_o.at[3], {"core": oc})

    def b_second():
        landed(er, r_b.at[0], two[0])
        landed(br, r_b.at[1], rings[0])
        for d in range(2):
            for sub in range(2):
                own = yb[3 + d, 64 * sub:64 * sub + 64] + br[d, 64 * sub:64 * sub + 64].astype(F32)
                if sub == d:
                    own = own + er[d].astype(F32)
                bs[2, d, 64 * sub:64 * sub + 64] = own.astype(BF)
            send(bs.at[2, d], parts_ref.at[c, 2 + d], s_b, r_b.at[3], two[d] | {"core": oc})

    last_block(1, block(0))
    a_step(0)
    y1(0)
    last_blocks(1, (block(1), block(2)))
    a_step(1)
    y1(1)
    last_blocks(1, (block(3), block(4)))
    last_blocks(1, (block(5), block(6)))
    last_block(1, block(7))
    y1(2)
    y1(3)
    y2(0)
    a_half(2, 0)
    a_half(2, 1)
    y2(1)
    a_step(3)
    y2(2)
    a_half(4, 0)
    a_half(4, 1)
    y3(0)
    b_far()
    y2(3)
    y3(1)
    b_third()
    a_step(5)
    a_half(6, 0)
    y3(2)
    a_half(6, 1)
    b_second()
    y3(3)
    b_near()
    a_last(0)
    a_last(1)
    blank.wait()
    kept[0].wait()
    landed(sums.at[oc], r_o.at[3], {"core": oc})
    landed(parts_ref.at[oc, 0:2], r_b.at[2], rings[0])
    landed(parts_ref.at[oc, 2:4], r_b.at[3], two[0])
    for n, there in enumerate(({"ylo": oy}, {"ylo": oy, "yhi": oh}, {"yhi": oh})):
        landed(parts_ref.at[c, n], r_o.at[n], there)
    for ref, sem in ((xb.at[0:3, 0, :, 0:128], s_xa), (fb.at[0:7, 0:4], s_x), (fb.at[0:4], s_d), (xb.at[0:7], s_z), (as_, s_a),
                     (y1s, s_y1), (y2s, s_y2), (es, s_e), (bs, s_b), (y2r.at[0, 0:3], s_o), (yb.at[7], s_g)):
        pltpu.make_async_remote_copy(
            src_ref=ref, dst_ref=ref, send_sem=sem, recv_sem=sem, device_id={"core": oc}, device_id_type=MESH).wait_send()


def per_device(factors, trials):
    dma = pltpu.SemaphoreType.DMA
    sums, parts = pl.pallas_call(
        kernel,
        out_shape=(jax.ShapeDtypeStruct((2, 128, 128), F32), jax.ShapeDtypeStruct((2, 4, 128, 128), BF)),
        in_specs=[pl.BlockSpec(memory_space=pl.ANY), pl.BlockSpec(memory_space=pl.ANY)],
        out_specs=(pl.BlockSpec(memory_space=pl.ANY),) * 2,
        scratch_shapes=[
            pltpu.VMEM((8, 8, 256, 256), BF),
            pltpu.VMEM((8, 2, 256, 256), BF),
            pltpu.VMEM((2, 256, 128), F32),
            pltpu.VMEM((2, 256, 128), BF),
            pltpu.VMEM((8, 2, 2, 128, 256), F32),
            pltpu.VMEM((2, 512, 512), F32),
            pltpu.VMEM((512, 512), BF),
            pltpu.VMEM((2, 7, 2, 128, 128), BF),
            pltpu.VMEM((2, 7, 2, 128, 128), BF),
            pltpu.VMEM((2, 8, 64, 128), BF),
            pltpu.VMEM((2, 8, 64, 128), BF),
            pltpu.VMEM((2, 8, 128, 128), BF),
            pltpu.VMEM((2, 8, 128, 128), BF),
            pltpu.VMEM((8, 128, 128), F32),
            pltpu.VMEM((2, 64, 128), BF),
            pltpu.VMEM((2, 64, 128), BF),
            pltpu.VMEM((3, 2, 128, 128), BF),
            pltpu.VMEM((2, 128, 128), BF),
            pltpu.VMEM((2, 128, 128), F32),
            pltpu.VMEM((2, 2, 128, 128), BF),
            pltpu.VMEM((128, 128), BF),
            dma((5,)), dma(()), dma((3,)), dma((4,)), dma(()), dma((12,)),
            dma(()), dma((6,)), dma(()), dma((7,)), dma(()), dma((7, 2)),
            dma(()), dma((4,)), dma(()), dma((4,)), dma(()), dma(()), dma((4,)), dma(()), dma(()), dma((4,)),
        ],
        compiler_params=pltpu.CompilerParams(
            collective_id=0, has_side_effects=True, vmem_limit_bytes=60000 * 1024),
    )(factors, trials)
    a, b, c, d = (parts[:, n].astype(F32) for n in range(4))
    return (sums + a) + (b + (c + d))


def solution(mesh):
    torus = Mesh(mesh.devices.reshape(NZ, 2, NX, 2, 2), ("z", "core", "x", "ylo", "yhi"))
    in_specs = (P(("z", "core", "yhi"), None, ("x", "ylo")), P(("x", "ylo"), None, ("z", "core")))
    out_specs = P(("x", "ylo"), "yhi", ("z", "core"))
    return jax.shard_map(
        per_device, mesh=torus, in_specs=in_specs, out_specs=out_specs, check_vma=False
    )
```
